512 devices in a mesh: zero: 8 (over x, core), cols: 64 (over z, y).
Axes of the slice: x: 4, y: 4, z: 16, core: 2. Of those that a mesh axis runs over, the one named last changes fastest.
Arguments:
- train_gate: bfloat16 [5120, 25600], P('zero', 'cols'), may hold values from -0.25 to 0.25
- low_gate: bfloat16 [5120, 64], P('zero'), may hold values from -0.078125 to 0.078125
- high_gate: bfloat16 [64, 25600], P(None, 'cols'), may hold values from -0.75 to 0.75
- train_up: bfloat16 [5120, 25600], P('zero', 'cols'), may hold values from -0.25 to 0.25
- low_up: bfloat16 [5120, 64], P('zero'), may hold values from -0.078125 to 0.078125
- high_up: bfloat16 [64, 25600], P(None, 'cols'), may hold values from -0.75 to 0.75
- norm_train: float32 [5120], P(('zero', 'cols')), may hold values from 0.25 to 1.75
- norm_step: float32 [5120], P(('zero', 'cols')), may hold values from -0.3 to 0.3
Outputs:
- ready_gate: bfloat16 [5120, 25600], P(None, 'cols')
- ready_up: bfloat16 [5120, 25600], P(None, 'cols')
- column_gate: float32 [25600], P('cols')
- column_up: float32 [25600], P('cols')
- serve_norm: bfloat16 [5120], replicated
The draws below stay inside these ranges and needn't reach their ends.
All inputs are finite; a program needn't handle non-finite values.
Results may differ from the reference program's by a relative error of at most 0.001.
Values may be sent and summed in bfloat16 or wider, within the bound.
A program may use at most 128 MiB of HBM per device.

```python
import jax
import jax.numpy as jnp
from jax import lax

D_MODEL = 5120
D_INNER = 25600
RANK = 64


def raised(entries, key, source, target, shards_of, factor):
    def block_of(dim):
        return (jnp.arange(entries.shape[dim]) // (entries.shape[dim] // shards_of)).reshape((-1,) + (1,) * (entries.ndim - 1 - dim))

    one_side = jax.random.permutation(key, shards_of)[block_of(target)]
    other_side = (block_of(target) + shards_of // 2) % shards_of
    return jnp.where((block_of(source) == one_side) | (block_of(source) == other_side), factor * entries, entries)


def levels(own_key, dims, split, smallest, high):
    def one(dim, parts):
        heights = jax.random.uniform(jax.random.fold_in(jax.random.fold_in(own_key, 6), dim), (parts,), jnp.float32, smallest / len(split), high / len(split))
        return jnp.repeat(jnp.exp(heights), dims[dim] // parts).reshape((-1,) + (1,) * (len(dims) - dim - 1))

    loudness = one(*split[0])
    for cut in split[1:]:
        loudness = loudness * one(*cut)
    return loudness


def normal_values(key, dims, deviation, reach, shards=(), dtype=jnp.bfloat16):
    entries = jax.random.normal(key, dims, jnp.float32) * deviation
    if len(shards) > 0:
        entries = levels(key, dims, shards, -0.22, 0.18) * entries
    return jnp.clip(entries, min=-reach, max=reach).astype(dtype)


def bell_draw_with(key, extent, width, limit, pieces, heavy, kind=jnp.bfloat16):
    drawn = width * jax.random.normal(key, extent, jnp.float32)
    if pieces:
        drawn = drawn * levels(key, extent, pieces, -0.22, 0.18)
    return jnp.clip(raised(drawn, jax.random.fold_in(key, 3), *heavy), -limit, limit).astype(kind)


def setup_inputs(seed: int = 0) -> dict:
    seeds = jax.random.split(jax.random.key(seed), 9)
    return {
        "train_gate": bell_draw_with(seeds[0], (D_MODEL, D_INNER), D_MODEL ** -0.5, 0.25, ((0, 8), (1, 64)), (0, 1, 64, 4.0)),
        "low_gate": normal_values(seeds[1], (D_MODEL, RANK), D_MODEL ** -0.5, 0.078125, ((0, 8),)),
        "high_gate": normal_values(seeds[2], (RANK, D_INNER), RANK ** -0.5, 0.75, ((1, 64),)),
        "train_up": bell_draw_with(seeds[3], (D_MODEL, D_INNER), D_MODEL ** -0.5, 0.25, ((0, 8), (1, 64)), (0, 1, 64, 4.0)),
        "low_up": normal_values(seeds[4], (D_MODEL, RANK), D_MODEL ** -0.5, 0.078125, ((0, 8),)),
        "high_up": normal_values(seeds[5], (RANK, D_INNER), RANK ** -0.5, 0.75, ((1, 64),)),
        "norm_train": jnp.clip(1.0 + 0.15 * jax.random.normal(seeds[6], (D_MODEL,), jnp.float32), 0.25, 1.75),
        "norm_step": jnp.clip(jax.random.uniform(seeds[7], (D_MODEL,), jnp.float32, -0.3, 0.3) * levels(seeds[7], (D_MODEL,), ((0, 512),), -0.4, 0.0), -0.3, 0.3),
    }


mix_rate = 2.0

def reference(train_gate, low_gate, high_gate, train_up, low_up, high_up, norm_train, norm_step):
    latest_gate = train_gate.astype(jnp.float32) + mix_rate * jnp.dot(low_gate, high_gate, preferred_element_type=jnp.float32)
    latest_up = train_up.astype(jnp.float32) + mix_rate * jnp.dot(low_up, high_up, preferred_element_type=jnp.float32)
    column_gate = jnp.sqrt(lax.optimization_barrier(jnp.sum(latest_gate * latest_gate, axis=0)))
    ready_gate = (latest_gate / column_gate).astype(jnp.bfloat16)
    column_up = jnp.sqrt(lax.optimization_barrier(jnp.sum(latest_up * latest_up, axis=0)))
    ready_up = (latest_up / column_up).astype(jnp.bfloat16)
    serve_norm = (norm_train + norm_step).astype(jnp.bfloat16)
    return (ready_gate, ready_up, column_gate, column_up, serve_norm)
```

```python
import functools

import jax
import jax.numpy as jnp
from jax import lax
from jax.experimental import pallas as pl
from jax.experimental.pallas import tpu as pltpu
from jax.sharding import PartitionSpec as P

F32, BF16 = jnp.float32, jnp.bfloat16
MESH = pl.DeviceIdType.MESH

NX, NC, NY, NZ = 4, 2, 4, 16
GROUP = NX * NC
D_MODEL, WIDE, RANK = 5120, 400, 64
ROWS = D_MODEL // GROUP
LANES = 128
STRIPS = ROWS // LANES
NCH = 2 * STRIPS
PAIRS = NCH // 2
MAIN, TAIL = 384, 16
STEP = 80
OWN, LEFT, RIGHT, FAR = 0, 1, 2, 3
PER = 10
NORM_ROWS = D_MODEL // LANES


def gather_kernel(
    tg, lg, hg, tu, lu, hu, nt, ns,
    out, col, norm,
    tv, lv, hv, ht, ntv, nsv,
    lat, part, spread, sums, ny, zr, zl, nscr,
    load_sem, sum_send, sum_recv,
    p_send, m_send, f_send, l_recv, r_recv, o_recv, d_send, d_recv,
    y_send, y_recv, zr_send, zr_recv, zl_send, zl_recv,
):
    me = lax.axis_index("zero")
    cols = lax.axis_index("cols")
    x, c = me // NC, me % NC
    z, y = cols // NY, cols % NY

    def chip(dx, core):
        return ((x + dx) % NX) * NC + core

    def at_x(dx, core):
        return (chip(dx, core), cols)

    def at_y(dy):
        return (me, z * NY + (y + dy) % NY)

    def at_z(dz):
        return (me, ((z + dz) % NZ) * NY + y)

    partner = at_x(0, 1 - c)
    plus, minus = at_x(1, c), at_x(NX - 1, c)
    group = [partner]
    for dx in range(1, NX):
        group += [at_x(dx, c), at_x(dx, 1 - c)]

    loads = [
        pltpu.make_async_copy(a, b, load_sem.at[i])
        for i, (a, b) in enumerate(
            ((hg, hv.at[0]), (hu, hv.at[1]), (lg, lv.at[0]), (lu, lv.at[1]),
             (tg, tv.at[0]), (tu, tv.at[1]), (nt, ntv), (ns, nsv))
        )
    ]
    for load in loads:
        load.start()

    barrier = pltpu.get_barrier_semaphore()
    peers = group + [at_y(1), at_y(NY - 1), at_z(1), at_z(NZ - 1)]
    for peer in peers:
        pl.semaphore_signal(barrier, inc=1, device_id=peer, device_id_type=MESH)

    for load in loads[:4]:
        load.wait()

    def dot(a, b):
        return jnp.dot(a, b, preferred_element_type=F32)

    for k in range(2):
        ht[k] = (hv[k].astype(F32).T * 2.0).astype(BF16)
    part[WIDE + TAIL:512, :] = jnp.zeros((512 - WIDE - TAIL, LANES), F32)

    for k in range(2):
        loads[4 + k].wait()
        for q in range(WIDE // STEP):
            r = slice(STEP * q, STEP * q + STEP)
            w = tv[k, r, :].astype(F32) + dot(ht[k, r, :], lv[k])
            lat[k, r, :] = w
            w = w * w
            s = w[:, 0:LANES]
            for t in range(1, STRIPS):
                s = s + w[:, LANES * t:LANES * t + LANES]
            if k == 0:
                part[r, :] = s
            elif r.stop <= MAIN:
                part[512 + r.start:512 + r.stop, :] = s
            else:
                part[512 + r.start:512 + MAIN, :] = s[:MAIN - r.start]
                part[WIDE:WIDE + TAIL, :] = s[MAIN - r.start:]
    loads[6].wait()
    loads[7].wait()

    lane = lax.broadcasted_iota(jnp.int32, (1, LANES), 1)
    gains = jnp.zeros((1, LANES), F32)
    for k in range(PER):
        gains = jnp.where(lane == (cols * PER + k) % LANES, ntv[k] + nsv[k], gains)

    mine = pl.multiple_of(me * 8, 8)
    sums[pl.ds(mine, 8), :] = jnp.concatenate(
        [jnp.sum(part[LANES * t:LANES * t + LANES, :].T, axis=0, keepdims=True) for t in range(7)]
        + [gains], axis=0)

    pl.semaphore_wait(barrier, len(peers))

    def sum_copy(k, peer, source):
        return pltpu.make_async_remote_copy(
            src_ref=sums.at[pl.ds(mine, 8), :],
            dst_ref=sums.at[pl.ds(mine, 8), :],
            send_sem=sum_send.at[k], recv_sem=sum_recv.at[source],
            device_id=peer, device_id_type=MESH)

    for k, peer in enumerate(group):
        sum_copy(k, peer, me).start()
    for k, peer in enumerate(group):
        sum_copy(k, peer, peer[0]).wait_recv()

    total = sums[0:8, :]
    for s in range(1, GROUP):
        total = total + sums[8 * s:8 * s + 8, :]
    column = jnp.sqrt(total)
    inverse = jnp.concatenate([1.0 / column, jnp.zeros((LANES - 8, LANES), F32)], axis=0).T

    def spread_out(k):
        for t in range(3):
            spread[k, LANES * t:LANES * t + LANES, :] = jnp.broadcast_to(
                inverse[:, 4 * k + t:4 * k + t + 1], (LANES, LANES))
        spread[k, MAIN:, :] = jnp.broadcast_to(
            inverse[TAIL * k:TAIL * k + TAIL, 3:4], (TAIL, LANES))

    def block(shard, j):
        return out.at[j // STRIPS, :, pl.ds(
            pl.multiple_of(shard * ROWS + (j % STRIPS) * LANES, LANES), LANES)]

    def remote(ref, send, recv, dev):
        return pltpu.make_async_remote_copy(
            src_ref=ref, dst_ref=ref, send_sem=send, recv_sem=recv,
            device_id=dev, device_id_type=MESH)

    source = [me, chip(NX - 1, c), chip(1, c), chip(2, c)]
    twin = [chip(0, 1 - c), chip(NX - 1, 1 - c), chip(1, 1 - c), chip(2, 1 - c)]

    def by_plus(j, shard=me):
        return remote(block(shard, j), p_send.at[j], l_recv.at[j], plus)

    def by_minus(j, shard=me):
        return remote(block(shard, j), m_send.at[j], r_recv.at[j], minus)

    def onward_plus(j, shard=source[LEFT]):
        return remote(block(shard, j), f_send.at[j], o_recv.at[j], plus)

    def onward_minus(j):
        return remote(block(source[RIGHT], j), f_send.at[j], o_recv.at[j], minus)

    def across(k, j, shards=source):
        return remote(block(shards[k], j), d_send.at[k * NCH + j], d_recv.at[k * NCH + j], partner)

    def make(k, t):
        j = k * STRIPS + t
        r = pl.ds(pl.multiple_of(t * LANES, LANES), LANES)
        o = pl.ds(pl.multiple_of(me * ROWS + t * LANES, LANES), LANES)
        out[k, :, o] = (lat[k, :, r] * spread[k]).astype(BF16)
        by_plus(j).start()
        by_minus(j).start()
        across(OWN, j).start()

    for k in range(2):
        spread_out(k)

        def make_step(t, _):
            make(k, t)
            return 0

        lax.fori_loop(0, STRIPS, make_step, 0)

    col[...] = jnp.concatenate(
        [jnp.concatenate([column[0:1], column[1:2], column[2:3], column[3:4]], axis=1),
         jnp.concatenate([column[4:5], column[5:6], column[6:7],
                          pltpu.roll(column, LANES - TAIL, axis=1)[3:4]], axis=1)], axis=0)

    row7 = jnp.concatenate([sums[8 * s + 7:8 * s + 8, :] for s in range(GROUP)], axis=0)
    lane8 = lax.broadcasted_iota(jnp.int32, (8, LANES), 1)
    for t in range(5):
        place = lane8 + LANES * t
        here = (place >= cols * PER) & (place < cols * PER + PER)
        ny[0, :, LANES * t:LANES * t + LANES] = jnp.where(here, row7, 0.0)

    def y_copy(src, dst, k, dev):
        return pltpu.make_async_remote_copy(
            src_ref=ny.at[src], dst_ref=ny.at[dst], send_sem=y_send.at[k], recv_sem=y_recv.at[k],
            device_id=dev, device_id_type=MESH)

    to_up, to_down, onward = y_copy(0, 1, 0, at_y(1)), y_copy(0, 2, 1, at_y(NY - 1)), y_copy(1, 3, 2, at_y(1))

    def z_right(src, s):
        return pltpu.make_async_remote_copy(
            src_ref=src, dst_ref=zr.at[s], send_sem=zr_send.at[s], recv_sem=zr_recv.at[s],
            device_id=at_z(1), device_id_type=MESH)

    def z_left(src, s):
        return pltpu.make_async_remote_copy(
            src_ref=src, dst_ref=zl.at[s], send_sem=zl_send.at[s], recv_sem=zl_recv.at[s],
            device_id=at_z(NZ - 1), device_id_type=MESH)

    to_up.start()
    to_down.start()

    def even(j):
        by_plus(j, source[LEFT]).wait_recv()
        onward_plus(j).start()
        across(LEFT, j).start()
        by_minus(j, source[RIGHT]).wait_recv()
        across(RIGHT, j).start()

    def odd(j):
        by_minus(j, source[RIGHT]).wait_recv()
        onward_minus(j).start()
        across(RIGHT, j).start()
        by_plus(j, source[LEFT]).wait_recv()
        across(LEFT, j).start()

    even(0)
    to_up.wait_recv()
    onward.start()
    odd(1)
    to_down.wait_recv()
    onward.wait_recv()
    onward.wait_send()
    to_up.wait_send()
    to_down.wait_send()
    ny[0] = ny[0] + ny[1] + (ny[2] + ny[3])
    z_right(ny.at[0], 0).start()
    z_left(ny.at[0], 0).start()

    def pair(q, _):
        s = 2 * q - 1
        even(2 * q)
        z_right(ny.at[0], s - 1).wait_recv()
        z_right(zr.at[s - 1], s).start()
        z_left(ny.at[0], s - 1).wait_recv()

        @pl.when(q < PAIRS - 1)
        def _():
            z_left(zl.at[s - 1], s).start()

        odd(2 * q + 1)
        z_right(ny.at[0], s).wait_recv()

        @pl.when(q < PAIRS - 1)
        def _():
            z_right(zr.at[s], s + 1).start()
            z_left(ny.at[0], s).wait_recv()
            z_left(zl.at[s], s + 1).start()

        return 0

    lax.fori_loop(1, PAIRS, pair, 0)

    gain = ny[0]
    for s in range(8):
        gain = gain + zr[s]
    for s in range(7):
        gain = gain + zl[s]
    for t in range(5):
        nscr[pl.ds(t, 8, stride=5), :] = gain[:, LANES * t:LANES * t + LANES]
    norm[...] = nscr[...].astype(BF16)

    def far_step(j, _):
        onward_plus(j, source[FAR]).wait_recv()
        across(FAR, j).start()
        return 0

    lax.fori_loop(0, NCH, far_step, 0)

    for k, peer in enumerate(group):
        sum_copy(k, peer, me).wait_send()

    def drain_z(s, _):
        z_right(ny.at[0], s).wait_send()

        @pl.when(s < 7)
        def _():
            z_left(ny.at[0], s).wait_send()

        return 0

    lax.fori_loop(0, 8, drain_z, 0)

    def drain_step(j, _):
        by_plus(j).wait_send()
        by_minus(j).wait_send()
        onward_plus(j).wait_send()
        for k in range(4):
            across(k, j).wait_send()
            across(k, j, twin).wait_recv()
        return 0

    lax.fori_loop(0, NCH, drain_step, 0)


def write_kernel(both, gate, up, sem):
    copies = []
    for k, dst in enumerate((gate, up)):
        for q in range(5):
            r = pl.ds(q * STEP, STEP)
            copies.append(pltpu.make_async_copy(both.at[k, r, :], dst.at[r, :], sem.at[5 * k + q]))
    for copy in copies:
        copy.start()
    for copy in copies:
        copy.wait()


def on_device(tg, lg, hg, tu, lu, hu, nt, ns):
    dma = pltpu.SemaphoreType.DMA
    hbm = pl.BlockSpec(memory_space=pltpu.HBM)
    vmem = pl.BlockSpec(memory_space=pltpu.VMEM)
    both, col, norm = pl.pallas_call(
        gather_kernel,
        name="gather_weights",
        out_shape=(
            pltpu.VMEM((2, WIDE, D_MODEL), BF16),
            jax.ShapeDtypeStruct((2, 512), F32),
            jax.ShapeDtypeStruct((NORM_ROWS, LANES), BF16),
        ),
        in_specs=[hbm] * 8,
        out_specs=(vmem, vmem, vmem),
        scratch_shapes=[
            pltpu.VMEM((2, WIDE, ROWS), BF16), pltpu.VMEM((2, RANK, ROWS), BF16),
            pltpu.VMEM((2, RANK, WIDE), BF16), pltpu.VMEM((2, WIDE, RANK), BF16),
            pltpu.SMEM((PER,), F32), pltpu.SMEM((PER,), F32),
            pltpu.VMEM((2, WIDE, ROWS), F32), pltpu.VMEM((7 * LANES, LANES), F32),
            pltpu.VMEM((2, WIDE, LANES), F32), pltpu.VMEM((GROUP * 8, LANES), F32),
            pltpu.VMEM((4, 8, 640), F32), pltpu.VMEM((8, 8, 640), F32), pltpu.VMEM((7, 8, 640), F32),
            pltpu.VMEM((NORM_ROWS, LANES), F32),
            dma((8,)), dma((GROUP - 1,)), dma((GROUP,)),
            dma((NCH,)), dma((NCH,)), dma((NCH,)), dma((NCH,)), dma((NCH,)), dma((NCH,)),
            dma((4 * NCH,)), dma((4 * NCH,)),
            dma((3,)), dma((4,)), dma((8,)), dma((8,)), dma((7,)), dma((7,)),
        ],
        compiler_params=pltpu.CompilerParams(
            collective_id=0, has_side_effects=True, vmem_limit_bytes=24 << 20),
    )(*(pltpu.with_memory_space_constraint(a, pltpu.HBM) for a in (tg.T, lg.T, hg, tu.T, lu.T, hu, nt, ns)))
    gate, up = pl.pallas_call(
        write_kernel,
        name="write_weights",
        out_shape=(jax.ShapeDtypeStruct((WIDE, D_MODEL), BF16),) * 2,
        in_specs=[vmem],
        out_specs=(hbm, hbm),
        scratch_shapes=[dma((10,))],
        compiler_params=pltpu.CompilerParams(vmem_limit_bytes=4 << 20),
    )(pltpu.with_memory_space_constraint(both, pltpu.VMEM))
    return gate.T, up.T, col[0, :WIDE], col[1, :WIDE], norm.reshape(D_MODEL)


def solution(mesh):
    return jax.shard_map(
        on_device,
        mesh=mesh,
        in_specs=(
            P("zero", "cols"), P("zero", None), P(None, "cols"),
            P("zero", "cols"), P("zero", None), P(None, "cols"),
            P(("zero", "cols")), P(("zero", "cols")),
        ),
        out_specs=(P(None, "cols"), P(None, "cols"), P("cols"), P("cols"), P()),
        check_vma=False,
    )
```

```python
import jax
import jax.numpy as jnp
from jax import lax
from jax.experimental import pallas as pl
from jax.experimental.pallas import tpu as pltpu
from jax.sharding import PartitionSpec as P

F32, BF16 = jnp.float32, jnp.bfloat16
MESH = pl.DeviceIdType.MESH

NX, NC, NY, NZ = 4, 2, 4, 16
GROUP = NX * NC
D_MODEL, WIDE, RANK = 5120, 400, 64
ROWS = D_MODEL // GROUP
LANES = 128
STRIPS = ROWS // LANES
MAIN, TAIL = 384, 16
STEP = 80
PER = 10
NORM_ROWS = D_MODEL // LANES

RAW = range(0, STRIPS)
LOW = range(STRIPS, STRIPS + 2)
UP = range(STRIPS + 2, 2 * STRIPS + 2)
PIECES = 2 * STRIPS + 2
BY_PLUS = (0, 2, 4, 5, 8, 10)
OWN, LEFT, RIGHT, FAR = 0, 1, 2, 3


def gather_kernel(
    tg, lg, hg, tu, lu, hu, nt, ns,
    out_g, out_u, col_g, col_u, norm,
    raw, low, tuv, luv, hv, ht, ntv, nsv,
    lat, part, spread, sums, ybuf, zbuf, gains, nscr,
    load_sem, here, y_token, z_token,
    sum_send, sum_recv, sum_d_send, sum_d_recv,
    p_send, m_send, f_send, l_recv, r_recv, o_recv, d_send, d_recv,
    y_send, y_recv, z_send, z_recv, g_send, g_recv,
):
    me = lax.axis_index("zero")
    cols = lax.axis_index("cols")
    x, c = me // NC, me % NC
    z, y = cols // NY, cols % NY

    def chip(dx, core):
        return ((x + dx) % NX) * NC + core

    def at_x(dx, core):
        return (chip(dx, core), cols)

    def at_y(dy):
        return (me, z * NY + (y + dy) % NY)

    def at_z(dz):
        return (me, ((z + dz) % NZ) * NY + y)

    def signal(sem, dev):
        pl.semaphore_signal(sem, inc=1, device_id=dev, device_id_type=MESH)

    def copy_to(src, dst, send, recv, dev):
        return pltpu.make_async_remote_copy(
            src_ref=src, dst_ref=dst, send_sem=send, recv_sem=recv,
            device_id=dev, device_id_type=MESH)

    def remote(ref, send, recv, dev):
        return copy_to(ref, ref, send, recv, dev)

    partner = at_x(0, 1 - c)
    plus, minus, far = at_x(1, c), at_x(NX - 1, c), at_x(2, c)
    rail = [plus, minus, far]

    def lanes(shard, at=0, n=ROWS):
        return pl.ds(pl.multiple_of(shard * ROWS + at, LANES), n)

    mine = lanes(me)

    loads = [
        pltpu.make_async_copy(a, b, load_sem.at[i])
        for i, (a, b) in enumerate(
            ((tg, raw.at[:, mine]), (hg, hv.at[0]), (lg, low.at[:, mine]),
             (hu, hv.at[1]), (lu, luv), (tu, tuv), (nt, ntv), (ns, nsv))
        )
    ]
    for load in loads:
        load.start()

    barrier = pltpu.get_barrier_semaphore()
    for peer in rail:
        signal(barrier, peer)

    @pl.when(c == 1)
    def _():
        for peer in (partner, at_y(1), at_y(NY - 1), at_z(1), at_z(NZ - 1)):
            signal(barrier, peer)

    source = [me, chip(NX - 1, c), chip(1, c), chip(2, c)]
    twin = [chip(0, 1 - c), chip(NX - 1, 1 - c), chip(1, 1 - c), chip(2, 1 - c)]

    def piece(shard, n):
        if n in RAW:
            return raw.at[:, lanes(shard, n * LANES, LANES)]
        if n in LOW:
            return low.at[pl.ds((n - STRIPS) * (RANK // 2), RANK // 2), lanes(shard)]
        return out_u.at[:, lanes(shard, (n - STRIPS - 2) * LANES, LANES)]

    def by_plus(n, k=OWN):
        return remote(piece(source[k], n), p_send.at[n], l_recv.at[n], plus)

    def by_minus(n, k=OWN):
        return remote(piece(source[k], n), m_send.at[n], r_recv.at[n], minus)

    def onward(n, k=None):
        k, dev = (LEFT if k is None else k, plus) if n in BY_PLUS else (RIGHT if k is None else k, minus)
        return remote(piece(source[k], n), f_send.at[n], o_recv.at[n], dev)

    def across(k, n, shards=source):
        i = k * PIECES + n
        return remote(piece(shards[k], n), d_send.at[i], d_recv.at[i], partner)

    def both_ways(n):
        by_plus(n).start()
        by_minus(n).start()

    def pass_on(n):
        def from_left():
            by_plus(n, LEFT).wait_recv()
            if n in BY_PLUS:
                onward(n).start()
            across(LEFT, n).start()

        def from_right():
            by_minus(n, RIGHT).wait_recv()
            if n not in BY_PLUS:
                onward(n).start()
            across(RIGHT, n).start()

        for step in (from_left, from_right) if n in BY_PLUS else (from_right, from_left):
            step()

    loads[0].wait()
    pl.semaphore_wait(barrier, 4 + 3 * c)
    both_ways(0)

    @pl.when(c == 0)
    def _():
        signal(here, partner)

    @pl.when(c == 1)
    def _():
        for peer in (at_y(1), at_y(NY - 1)):
            signal(y_token, peer)
        for peer in (at_z(1), at_z(NZ - 1)):
            signal(z_token.at[0], peer)

    def dot(a, b):
        return jnp.dot(a, b, preferred_element_type=F32)

    loads[1].wait()
    loads[3].wait()
    for k in range(2):
        ht[k] = (hv[k].astype(F32).T * 2.0).astype(BF16)
    part[WIDE + TAIL:512, :] = jnp.zeros((512 - WIDE - TAIL, LANES), F32)

    for k in range(2):
        loads[2 + 2 * k].wait()
        if k == 1:
            loads[5].wait()
        for q in range(WIDE // STEP):
            r = slice(STEP * q, STEP * q + STEP)
            if k == 0:
                w = raw[r, mine].astype(F32) + dot(ht[0, r, :], low[:, mine])
            else:
                w = tuv[r, :].astype(F32) + dot(ht[1, r, :], luv[...])
                lat[r, :] = w
            w = w * w
            s = w[:, 0:LANES]
            for t in range(1, STRIPS):
                s = s + w[:, LANES * t:LANES * t + LANES]
            if k == 0:
                part[r, :] = s
            elif r.stop <= MAIN:
                part[512 + r.start:512 + r.stop, :] = s
            else:
                part[512 + r.start:512 + MAIN, :] = s[:MAIN - r.start]
                part[WIDE:WIDE + TAIL, :] = s[MAIN - r.start:]
    loads[6].wait()
    loads[7].wait()

    lane = lax.broadcasted_iota(jnp.int32, (1, LANES), 1)
    own_gains = jnp.zeros((1, LANES), F32)
    for k in range(PER):
        own_gains = jnp.where(lane == (cols * PER + k) % LANES, ntv[k] + nsv[k], own_gains)

    sums[me] = jnp.concatenate(
        [jnp.sum(part[LANES * t:LANES * t + LANES, :].T, axis=0, keepdims=True) for t in range(7)]
        + [own_gains], axis=0)

    def sum_copy(i, peer, owner):
        return remote(sums.at[owner], sum_send.at[i], sum_recv.at[i], peer)

    def sum_across(k, owners=source):
        return remote(sums.at[owners[k]], sum_d_send.at[k], sum_d_recv.at[k], partner)

    for i, peer in enumerate(rail):
        sum_copy(i, peer, me).start()
    for n in (*LOW, *RAW[1:]):
        both_ways(n)

    @pl.when(c == 1)
    def _():
        pl.semaphore_wait(here, 1)

    sum_across(OWN).start()
    for n in (*RAW, *LOW):
        across(OWN, n).start()

    pass_on(0)
    for i, k in enumerate((LEFT, RIGHT, FAR)):
        sum_copy(i, plus, source[k]).wait_recv()
        sum_across(k).start()

    @pl.when(c == 1)
    def _():
        pl.semaphore_wait(z_token.at[0], 2)
        for peer in (at_z(2), at_z(NZ - 2)):
            signal(z_token.at[1], peer)
        pl.semaphore_wait(y_token, 2)

    for n in (*LOW, *RAW[1:]):
        pass_on(n)

    for k in range(4):
        sum_across(k, twin).wait_recv()

    total = sums[0]
    for s in range(1, GROUP):
        total = total + sums[s]
    column = jnp.sqrt(total)
    inverse = jnp.concatenate([1.0 / column, jnp.zeros((LANES - 8, LANES), F32)], axis=0).T

    def spread_out(k):
        for t in range(3):
            spread[k, LANES * t:LANES * t + LANES, :] = jnp.broadcast_to(
                inverse[:, 4 * k + t:4 * k + t + 1], (LANES, LANES))
        spread[k, MAIN:, :] = jnp.broadcast_to(
            inverse[TAIL * k:TAIL * k + TAIL, 3:4], (TAIL, LANES))

    spread_out(1)
    for n in UP:
        t = n - STRIPS - 2
        out_u[:, lanes(me, t * LANES, LANES)] = (lat[:, t * LANES:t * LANES + LANES] * spread[1]).astype(BF16)
        both_ways(n)
        across(OWN, n).start()
    spread_out(0)

    col_g[...] = jnp.concatenate(
        [column[0:1], column[1:2], column[2:3], column[3:4]], axis=1)[:, :WIDE]
    col_u[...] = jnp.concatenate(
        [column[4:5], column[5:6], column[6:7], pltpu.roll(column, LANES - TAIL, axis=1)[3:4]], axis=1)[:, :WIDE]

    y_copies = [copy_to(ybuf.at[0], ybuf.at[i + 1], y_send.at[i], y_recv.at[i], at_y(dy))
                for i, dy in enumerate((1, NY - 1, 2))]

    def z_copy(d):
        return copy_to(zbuf.at[0], zbuf.at[d], z_send.at[d - 1], z_recv.at[d - 1], at_z(d))

    @pl.when(c == 1)
    def _():
        ybuf[0] = jnp.concatenate([sums[s][7:8, :] for s in range(GROUP)], axis=0)
        for copy in y_copies:
            copy.start()
        pl.semaphore_wait(z_token.at[1], 2)
        for peer in (at_z(4), at_z(NZ - 4)):
            signal(z_token.at[2], peer)

    for n in (*RAW[:1], *LOW, *RAW[1:]):
        onward(n, FAR).wait_recv()
        across(FAR, n).start()

    @pl.when(c == 1)
    def _():
        for copy in y_copies:
            copy.wait_recv()
        zbuf[0] = (ybuf[0] + ybuf[1]) + (ybuf[2] + ybuf[3])
        pl.semaphore_wait(z_token.at[2], 2)
        for d in range(1, NZ):
            z_copy(d).start()

    for n in (*RAW, *LOW):
        for k in range(4):
            across(k, n, twin).wait_recv()

    def finish(i, _):
        w = pl.ds(pl.multiple_of(i * 2 * LANES, 2 * LANES), 2 * LANES)
        for q in range(WIDE // STEP):
            r = slice(STEP * q, STEP * q + STEP)
            s = spread[0, r, :]
            v = raw[r, w].astype(F32) + dot(ht[0, r, :], low[:, w])
            out_g[r, w] = (v * jnp.concatenate([s, s], axis=1)).astype(BF16)
        return 0

    lax.fori_loop(0, D_MODEL // (2 * LANES), finish, 0)

    for n in UP:
        pass_on(n)
    for n in UP[:-2]:
        onward(n, FAR).wait_recv()
        across(FAR, n).start()

    def gains_across():
        return remote(gains, g_send.at[0], g_recv.at[0], partner)

    @pl.when(c == 1)
    def _():
        for d in range(1, NZ):
            z_copy(d).wait_recv()
        lane8 = lax.broadcasted_iota(jnp.int32, (8, LANES), 1)
        tiles = [jnp.zeros((8, LANES), F32) for _ in range(5)]
        for d in range(NZ):
            start = ((z + NZ - d) % NZ) * NY * PER
            tile = zbuf[d]
            for t in range(5):
                place = lane8 + LANES * t
                tiles[t] = jnp.where((place >= start) & (place < start + NY * PER), tile, tiles[t])
        for t in range(5):
            gains[:, LANES * t:LANES * t + LANES] = tiles[t]
        gains_across().start()

    for n in UP[-2:]:
        onward(n, FAR).wait_recv()
        across(FAR, n).start()

    @pl.when(c == 0)
    def _():
        gains_across().wait_recv()

    for t in range(5):
        nscr[pl.ds(t, 8, stride=5), :] = gains[:, LANES * t:LANES * t + LANES]
    norm[...] = nscr[...].astype(BF16)

    @pl.when(c == 1)
    def _():
        gains_across().wait_send()
        for copy in y_copies:
            copy.wait_send()
        for d in range(1, NZ):
            z_copy(d).wait_send()

    for i, peer in enumerate(rail):
        sum_copy(i, peer, me).wait_send()
    for k in range(4):
        sum_across(k).wait_send()
    for n in range(PIECES):
        by_plus(n).wait_send()
        by_minus(n).wait_send()
        onward(n).wait_send()
        for k in range(4):
            across(k, n).wait_send()
            if n in UP:
                across(k, n, twin).wait_recv()


def write_kernel(*refs):
    n = (len(refs) - 1) // 2
    sources, targets, sem = refs[:n], refs[n:2 * n], refs[2 * n]
    copies = []
    for src, dst in zip(sources, targets):
        tall = src.shape[0] == WIDE
        for q in range(WIDE // STEP if tall else 1):
            r = pl.ds(q * STEP, STEP) if tall else slice(None)
            copies.append(pltpu.make_async_copy(src.at[r, :], dst.at[r, :], sem.at[len(copies)]))
    for copy in copies:
        copy.start()
    for copy in copies:
        copy.wait()


def on_device(tg, lg, hg, tu, lu, hu, nt, ns):
    dma, regular = pltpu.SemaphoreType.DMA, pltpu.SemaphoreType.REGULAR
    hbm = pl.BlockSpec(memory_space=pltpu.HBM)
    vmem = pl.BlockSpec(memory_space=pltpu.VMEM)
    results = (
        ((WIDE, D_MODEL), BF16), ((WIDE, D_MODEL), BF16),
        ((1, WIDE), F32), ((1, WIDE), F32), ((NORM_ROWS, LANES), BF16),
    )
    made = pl.pallas_call(
        gather_kernel,
        name="gather_weights",
        out_shape=tuple(pltpu.VMEM(*r) for r in results),
        in_specs=[hbm] * 8,
        out_specs=(vmem,) * 5,
        scratch_shapes=[
            pltpu.VMEM((WIDE, D_MODEL), BF16), pltpu.VMEM((RANK, D_MODEL), BF16),
            pltpu.VMEM((WIDE, ROWS), BF16), pltpu.VMEM((RANK, ROWS), BF16),
            pltpu.VMEM((2, RANK, WIDE), BF16), pltpu.VMEM((2, WIDE, RANK), BF16),
            pltpu.SMEM((PER,), F32), pltpu.SMEM((PER,), F32),
            pltpu.VMEM((WIDE, ROWS), F32), pltpu.VMEM((7 * LANES, LANES), F32),
            pltpu.VMEM((2, WIDE, LANES), F32), pltpu.VMEM((GROUP, 8, LANES), F32),
            pltpu.VMEM((NY, 8, LANES), F32), pltpu.VMEM((NZ, 8, LANES), F32),
            pltpu.VMEM((8, 5 * LANES), F32), pltpu.VMEM((NORM_ROWS, LANES), F32),
            dma((8,)), regular, regular, regular((3,)),
            dma((3,)), dma((3,)), dma((4,)), dma((4,)),
            *[dma((PIECES,))] * 6, dma((4 * PIECES,)), dma((4 * PIECES,)),
            dma((3,)), dma((3,)), dma((NZ - 1,)), dma((NZ - 1,)), dma((1,)), dma((1,)),
        ],
        compiler_params=pltpu.CompilerParams(
            collective_id=0, has_side_effects=True, vmem_limit_bytes=24 << 20),
    )(*(pltpu.with_memory_space_constraint(a, pltpu.HBM) for a in (tg.T, lg.T, hg, tu.T, lu.T, hu, nt, ns)))
    gate, up, col_g, col_u, norm = pl.pallas_call(
        write_kernel,
        name="write_results",
        out_shape=tuple(jax.ShapeDtypeStruct(*r) for r in results),
        in_specs=[vmem] * 5,
        out_specs=(hbm,) * 5,
        scratch_shapes=[dma((13,))],
        compiler_params=pltpu.CompilerParams(vmem_limit_bytes=4 << 20),
    )(*(pltpu.with_memory_space_constraint(a, pltpu.VMEM) for a in made))
    return gate.T, up.T, col_g.reshape(WIDE), col_u.reshape(WIDE), norm.reshape(D_MODEL)


def solution(mesh):
    return jax.shard_map(
        on_device,
        mesh=mesh,
        in_specs=(
            P("zero", "cols"), P("zero", None), P(None, "cols"),
            P("zero", "cols"), P("zero", None), P(None, "cols"),
            P(("zero", "cols")), P(("zero", "cols")),
        ),
        out_specs=(P(None, "cols"), P(None, "cols"), P("cols"), P("cols"), P()),
        check_vma=False,
    )
```

```python
import jax
import jax.numpy as jnp
from jax import lax
from jax.experimental import pallas as pl
from jax.experimental.pallas import tpu as pltpu
from jax.sharding import PartitionSpec as P

F32, BF16 = jnp.float32, jnp.bfloat16
MESH = pl.DeviceIdType.MESH

NX, NC, NY, NZ = 4, 2, 4, 16
GROUP = NX * NC
D_MODEL, WIDE, RANK = 5120, 400, 64
ROWS = D_MODEL // GROUP
LANES = 128
STRIPS = ROWS // LANES
MAIN, TAIL = 384, 16
STEP = 80
PER = 10
NORM_ROWS = D_MODEL // LANES

RAW = range(0, STRIPS)
LOW = range(STRIPS, STRIPS + 2)
UP = range(STRIPS + 2, 2 * STRIPS + 2)
PIECES = 2 * STRIPS + 2
BY_PLUS = (0, 2, 4, 5, 8, 10)
OWN, LEFT, RIGHT, FAR = 0, 1, 2, 3


def gather_kernel(
    tg, lg, hg, tu, lu, hu, nt, ns,
    out_g, out_u, col_g, col_u, norm,
    raw, low, tuv, luv, hv, ht, ntv, nsv,
    lat, part, spread, sums, gbuf, ybuf, zbuf, nscr,
    load_sem, here, y_token, z_token,
    send, l_recv, r_recv, far_recv, d_recv, small_recv, n_send,
):
    me = lax.axis_index("zero")
    cols = lax.axis_index("cols")
    x, c = me // NC, me % NC
    z, y = cols // NY, cols % NY

    def chip(dx, core):
        return ((x + dx) % NX) * NC + core

    def at_x(dx, core):
        return (chip(dx, core), cols)

    def at_y(dy):
        return (me, z * NY + (y + dy) % NY)

    def at_z(dz):
        return (me, ((z + dz) % NZ) * NY + y)

    def signal(sem, dev):
        pl.semaphore_signal(sem, inc=1, device_id=dev, device_id_type=MESH)

    def copy_to(src, dst, send, recv, dev):
        return pltpu.make_async_remote_copy(
            src_ref=src, dst_ref=dst, send_sem=send, recv_sem=recv,
            device_id=dev, device_id_type=MESH)

    def remote(ref, send, recv, dev):
        return copy_to(ref, ref, send, recv, dev)

    partner = at_x(0, 1 - c)
    plus, minus, far = at_x(1, c), at_x(NX - 1, c), at_x(2, c)
    rail = [plus, minus, far]

    def lanes(shard, at=0, n=ROWS):
        return pl.ds(pl.multiple_of(shard * ROWS + at, LANES), n)

    mine = lanes(me)

    head = me == 0
    barrier = pltpu.get_barrier_semaphore()
    for peer in rail:
        signal(barrier, peer)

    @pl.when(c == 1)
    def _():
        signal(barrier, partner)

    loads = [
        pltpu.make_async_copy(a, b, load_sem.at[i])
        for i, (a, b) in enumerate(
            ((tg, raw.at[:, mine]), (nt, ntv), (ns, nsv), (hg, hv.at[0]), (lg, low.at[:, mine]),
             (hu, hv.at[1]), (lu, luv), (tu, tuv))
        )
    ]
    for load in loads:
        load.start()

    for dy in (1, NY - 1):
        @pl.when(head & (y != 0))
        def _(dy=dy):
            signal(barrier, at_y(dy))

    for dz in (1, NZ - 1):
        @pl.when(head & ((z + dz) % NZ != 0))
        def _(dz=dz):
            signal(barrier, at_z(dz))

    source = [me, chip(NX - 1, c), chip(1, c), chip(2, c)]

    def piece(shard, n):
        if n in RAW:
            return raw.at[:, lanes(shard, n * LANES, LANES)]
        if n in LOW:
            return low.at[pl.ds((n - STRIPS) * (RANK // 2), RANK // 2), lanes(shard)]
        return out_u.at[:, lanes(shard, (n - STRIPS - 2) * LANES, LANES)]

    def sent(n):
        return send.at[0 if n in RAW else 1 if n in LOW else 2]

    def by_plus(n, k=OWN):
        return remote(piece(source[k], n), sent(n), l_recv.at[n], plus)

    def by_minus(n, k=OWN):
        return remote(piece(source[k], n), sent(n), r_recv.at[n], minus)

    def onward(n, k=None):
        k, dev = (LEFT if k is None else k, plus) if n in BY_PLUS else (RIGHT if k is None else k, minus)
        return remote(piece(source[k], n), sent(n), far_recv.at[0 if n in RAW else 1 if n in LOW else n - STRIPS], dev)

    def across(k, n):
        kind = (0 if n in RAW else 1) + (2 if k == FAR else 0) if n not in UP else 4
        return remote(piece(source[k], n), sent(n), d_recv.at[kind], partner)

    def crossed(ref, kind):
        return remote(ref, send.at[0], d_recv.at[kind], partner)

    def both_ways(n):
        by_plus(n).start()
        by_minus(n).start()

    def pass_on(n, now=True):
        def from_left():
            by_plus(n, LEFT).wait_recv()
            if n in BY_PLUS:
                onward(n).start()
            if now:
                across(LEFT, n).start()

        def from_right():
            by_minus(n, RIGHT).wait_recv()
            if n not in BY_PLUS:
                onward(n).start()
            if now:
                across(RIGHT, n).start()

        for step in (from_left, from_right) if n in BY_PLUS else (from_right, from_left):
            step()

    loads[1].wait()
    loads[2].wait()
    row8 = lax.broadcasted_iota(jnp.int32, (8, LANES), 0)
    lane8 = lax.broadcasted_iota(jnp.int32, (8, LANES), 1)
    tile = jnp.zeros((8, LANES), F32)
    for k in range(PER):
        tile = jnp.where(lane8 == (cols * PER + k) % LANES, ntv[k] + nsv[k], tile)
    gbuf[x] = jnp.where(row8 == me, tile, 0.0)

    def gain_copy(i):
        return copy_to(gbuf.at[i], gbuf.at[i], send.at[3], small_recv.at[0], (c, cols))

    loads[0].wait()
    met = jnp.where(y % 2 == 0, 2, 1) + jnp.where(z == 0, 0, 2)
    pl.semaphore_wait(barrier, 4 - c + jnp.where(head, met, 0))
    for i in range(1, NX):
        @pl.when(x == i)
        def _(i=i):
            gain_copy(i).start()
    both_ways(0)

    @pl.when(c == 0)
    def _():
        signal(here, partner)

    @pl.when(head & (y == 0))
    def _():
        for peer in (at_y(1), at_y(NY - 1)):
            signal(y_token.at[0], peer)

    @pl.when(head & (z != 0))
    def _():
        for peer in (at_z(1), at_z(NZ - 1)):
            signal(z_token.at[0], peer)

    def dot(a, b):
        return jnp.dot(a, b, preferred_element_type=F32)

    loads[3].wait()
    loads[5].wait()
    for k in range(2):
        ht[k] = (hv[k].astype(F32).T * 2.0).astype(BF16)
    part[WIDE + TAIL:512, :] = jnp.zeros((512 - WIDE - TAIL, LANES), F32)

    for k in range(2):
        loads[4 + 2 * k].wait()
        if k == 1:
            loads[7].wait()
        for q in range(WIDE // STEP):
            r = slice(STEP * q, STEP * q + STEP)
            if k == 0:
                w = raw[r, mine].astype(F32) + dot(ht[0, r, :], low[:, mine])
            else:
                w = tuv[r, :].astype(F32) + dot(ht[1, r, :], luv[...])
                lat[r, :] = w
            w = w * w
            s = w[:, 0:LANES]
            for t in range(1, STRIPS):
                s = s + w[:, LANES * t:LANES * t + LANES]
            if k == 0:
                part[r, :] = s
            elif r.stop <= MAIN:
                part[512 + r.start:512 + r.stop, :] = s
            else:
                part[512 + r.start:512 + MAIN, :] = s[:MAIN - r.start]
                part[WIDE:WIDE + TAIL, :] = s[MAIN - r.start:]

    sums[c * NX + x] = jnp.concatenate(
        [jnp.sum(part[LANES * t:LANES * t + LANES, :].T, axis=0, keepdims=True) for t in range(7)]
        + [jnp.zeros((1, LANES), F32)], axis=0)

    def sum_copy(peer, recv):
        return remote(sums.at[c * NX + x], send.at[4], small_recv.at[recv], peer)

    for peer in rail:
        sum_copy(peer, 1).start()
    for n in (*LOW, *RAW[1:]):
        both_ways(n)

    def tokens(step):
        for peer in (at_z(1 << step), at_z(NZ - (1 << step))):
            signal(z_token.at[step], peer)

    @pl.when(head & (z != 0))
    def _():
        pl.semaphore_wait(z_token.at[0], 2)
        tokens(1)
        pl.semaphore_wait(z_token.at[1], 2)
        tokens(2)

    def first_tokens():
        pl.semaphore_wait(z_token.at[0], 2)
        tokens(0)
        tokens(1)

    @pl.when(head & (cols == 0))
    def _():
        first_tokens()

    eager = (cols == 0) & (c == 1)

    @pl.when(eager)
    def _():
        for n in (0, *LOW, *RAW[1:]):
            pass_on(n, False)

    @pl.when(c == 1)
    def _():
        pl.semaphore_wait(here, 1)

    def gains_in():
        return remote(gbuf.at[pl.ds(0, 3)], send.at[3], small_recv.at[0], partner)

    def rail_gains():
        return (gbuf[0] + gbuf[1]) + (gbuf[2] + gbuf[3])

    def gains_over():
        return copy_to(gbuf.at[5], gbuf.at[4], send.at[3], small_recv.at[2], partner)

    @pl.when(me == 1)
    def _():
        gains_in().wait_recv()
        gbuf[5] = rail_gains()
        gains_over().start()

    remote(sums.at[pl.ds(0, 3)], send.at[4], small_recv.at[1], partner).wait_recv()
    rail_sums = remote(sums.at[pl.ds(c * NX, NX)], send.at[5], small_recv.at[3], partner)
    rail_sums.start()
    own_raw = remote(raw.at[:, mine], send.at[0], d_recv.at[0], partner)
    own_low = remote(low.at[:, mine], send.at[1], d_recv.at[1], partner)
    own_raw.start()
    own_low.start()
    remote(sums.at[pl.ds((1 - c) * NX, NX)], send.at[5], small_recv.at[3], partner).wait_recv()

    total = sums[0]
    for s in range(1, GROUP):
        total = total + sums[s % NC * NX + s // NC]
    column = jnp.sqrt(total)
    inverse = jnp.concatenate([1.0 / column, jnp.zeros((LANES - 8, LANES), F32)], axis=0).T

    def spread_out(k):
        for t in range(3):
            spread[k, LANES * t:LANES * t + LANES, :] = jnp.broadcast_to(
                inverse[:, 4 * k + t:4 * k + t + 1], (LANES, LANES))
        spread[k, MAIN:, :] = jnp.broadcast_to(
            inverse[TAIL * k:TAIL * k + TAIL, 3:4], (TAIL, LANES))

    spread_out(1)
    for n in UP:
        t = n - STRIPS - 2
        out_u[:, lanes(me, t * LANES, LANES)] = (lat[:, t * LANES:t * LANES + LANES] * spread[1]).astype(BF16)
        both_ways(n)
        across(OWN, n).start()
    spread_out(0)

    col_g[...] = jnp.concatenate(
        [column[0:1], column[1:2], column[2:3], column[3:4]], axis=1)[:, :WIDE]
    col_u[...] = jnp.concatenate(
        [column[4:5], column[5:6], column[6:7], pltpu.roll(column, LANES - TAIL, axis=1)[3:4]], axis=1)[:, :WIDE]

    y_copies = [copy_to(ybuf.at[0], ybuf.at[i + 1], send.at[6], small_recv.at[4], at_y(dy))
                for i, dy in enumerate((1, NY - 1, 2))]

    def y_all():
        return remote(ybuf.at[pl.ds(0, 3)], send.at[6], small_recv.at[4], partner)

    def z_copy(d):
        return copy_to(zbuf.at[0], zbuf.at[d], send.at[7], small_recv.at[5], at_z(d))

    def z_all():
        return remote(zbuf.at[pl.ds(0, NZ - 1)], send.at[7], small_recv.at[5], partner)

    @pl.when(head & (y % 2 == 1))
    def _():
        pl.semaphore_wait(y_token.at[0], 1)
        for peer in (at_y(1), at_y(NY - 1)):
            signal(y_token.at[1], peer)

    @pl.when(head & (y % 2 == 0))
    def _():
        pl.semaphore_wait(y_token.at[1], 2)

    @pl.when(head)
    def _():
        gains_in().wait_recv()
        gains_over().wait_recv()
        ybuf[0] = rail_gains() + gbuf[4]
        for copy in y_copies:
            copy.start()

    @pl.when(head & (z == 0) & (y != 0))
    def _():
        first_tokens()

    def pass_group(group):
        @pl.when(jnp.logical_not(eager))
        def _():
            for n in group:
                pass_on(n)

    pass_group((0, *LOW, *RAW[1:3]))

    @pl.when(head & (z == 0))
    def _():
        pl.semaphore_wait(z_token.at[1], 2)
        tokens(2)

    @pl.when(head)
    def _():
        y_all().wait_recv()
        zbuf[0] = (ybuf[0] + ybuf[1]) + (ybuf[2] + ybuf[3])

    def z_wave():
        pl.semaphore_wait(z_token.at[2], 2)
        for d in range(1, NZ):
            z_copy(d).start()

    @pl.when(head & (z != 0))
    def _():
        z_wave()

    pass_group(RAW[3:])

    @pl.when(eager)
    def _():
        for k in (LEFT, RIGHT):
            for n in (*RAW, *LOW):
                across(k, n).start()

    crossed(raw.at[:, pl.ds(0, 3 * ROWS)], 0).wait_recv()
    crossed(low.at[:, pl.ds(0, 3 * ROWS)], 1).wait_recv()

    def finish(shard):
        w = lanes(shard)
        for q in range(WIDE // STEP):
            r = slice(STEP * q, STEP * q + STEP)
            s = spread[0, r, :]
            v = raw[r, w].astype(F32) + dot(ht[0, r, :], low[:, w])
            out_g[r, w] = (v * jnp.concatenate([s] * STRIPS, axis=1)).astype(BF16)

    def finish_near(i, _):
        d = i // NC
        finish(chip(d + d // 2, i % NC))
        return 0

    lax.fori_loop(0, 3 * NC, finish_near, 0)

    @pl.when(head & (z == 0))
    def _():
        z_wave()

    for n in UP[:2]:
        pass_on(n)

    def norm_copy(i, dev):
        return remote(norm, n_send.at[i], small_recv.at[7 if i == 3 else 6], dev)

    @pl.when(head)
    def _():
        z_all().wait_recv()
        tiles = [jnp.zeros((8, LANES), F32) for _ in range(5)]
        for d in range(NZ):
            start = ((z + NZ - d) % NZ) * NY * PER
            for t in range(5):
                place = lane8 + LANES * t
                tiles[t] = jnp.where((place >= start) & (place < start + NY * PER), zbuf[d], tiles[t])
        for t in range(5):
            nscr[pl.ds(t, 8, stride=5), :] = tiles[t]
        norm[...] = nscr[...].astype(BF16)

    for n in UP[2:3]:
        pass_on(n)

    @pl.when(head)
    def _():
        for i, dev in enumerate((*rail, partner)):
            norm_copy(i, dev).start()

    for n in UP[3:]:
        pass_on(n)

    far_lanes = lanes(source[FAR])
    remote(raw.at[:, far_lanes], send.at[0], far_recv.at[0], plus).wait_recv()
    remote(raw.at[:, far_lanes], send.at[0], d_recv.at[2], partner).start()
    remote(low.at[:, far_lanes], send.at[1], far_recv.at[1], plus).wait_recv()
    remote(low.at[:, far_lanes], send.at[1], d_recv.at[3], partner).start()
    crossed(raw.at[:, far_lanes], 2).wait_recv()
    crossed(low.at[:, far_lanes], 3).wait_recv()

    def finish_far(i, _):
        finish(chip(2, i))
        return 0

    lax.fori_loop(0, NC, finish_far, 0)

    @pl.when((c == 0) & jnp.logical_not(head))
    def _():
        norm_copy(0, plus).wait_recv()
        norm_copy(3, partner).start()

    rail_sums.wait_send()
    remote(sums.at[pl.ds(0, 3)], send.at[4], small_recv.at[1], partner).wait_send()

    @pl.when((x > 0) | (me == 1))
    def _():
        gains_over().wait_send()

    @pl.when(head)
    def _():
        y_all().wait_send()
        z_all().wait_send()

    for n in UP[:-1]:
        onward(n, FAR).wait_recv()
        across(FAR, n).start()

    @pl.when(c == 1)
    def _():
        norm_copy(3, partner).wait_recv()

    @pl.when(c == 0)
    def _():
        norm_copy(3, partner).wait_send()

    @pl.when(head)
    def _():
        for i, dev in enumerate(rail):
            norm_copy(i, dev).wait_send()

    crossed(raw.at[:, pl.ds(0, 7 * ROWS)], 0).wait_send()
    remote(low.at[:, pl.ds(0, 7 * ROWS)], send.at[1], d_recv.at[1], partner).wait_send()

    for n in UP[-1:]:
        onward(n, FAR).wait_recv()
        across(FAR, n).start()
    remote(out_u.at[:, pl.ds(0, 7 * ROWS)], send.at[2], d_recv.at[4], partner).wait_send()
    crossed(out_u.at[:, pl.ds(0, 4 * ROWS)], 4).wait_recv()


def write_kernel(*refs):
    n = (len(refs) - 1) // 2
    sources, targets, sem = refs[:n], refs[n:2 * n], refs[2 * n]
    copies = []
    for src, dst in zip(sources, targets):
        tall = src.shape[0] == WIDE
        for q in range(WIDE // STEP if tall else 1):
            r = pl.ds(q * STEP, STEP) if tall else slice(None)
            copies.append(pltpu.make_async_copy(src.at[r, :], dst.at[r, :], sem.at[len(copies)]))
    for copy in copies:
        copy.start()
    for copy in copies:
        copy.wait()


def on_device(tg, lg, hg, tu, lu, hu, nt, ns):
    dma, regular = pltpu.SemaphoreType.DMA, pltpu.SemaphoreType.REGULAR
    hbm = pl.BlockSpec(memory_space=pltpu.HBM)
    vmem = pl.BlockSpec(memory_space=pltpu.VMEM)
    results = (
        ((WIDE, D_MODEL), BF16), ((WIDE, D_MODEL), BF16),
        ((1, WIDE), F32), ((1, WIDE), F32), ((NORM_ROWS, LANES), BF16),
    )
    made = pl.pallas_call(
        gather_kernel,
        name="gather_weights",
        out_shape=tuple(pltpu.VMEM(*r) for r in results),
        in_specs=[hbm] * 8,
        out_specs=(vmem,) * 5,
        scratch_shapes=[
            pltpu.VMEM((WIDE, D_MODEL), BF16), pltpu.VMEM((RANK, D_MODEL), BF16),
            pltpu.VMEM((WIDE, ROWS), BF16), pltpu.VMEM((RANK, ROWS), BF16),
            pltpu.VMEM((2, RANK, WIDE), BF16), pltpu.VMEM((2, WIDE, RANK), BF16),
            pltpu.SMEM((PER,), F32), pltpu.SMEM((PER,), F32),
            pltpu.VMEM((WIDE, ROWS), F32), pltpu.VMEM((7 * LANES, LANES), F32),
            pltpu.VMEM((2, WIDE, LANES), F32), pltpu.VMEM((GROUP, 8, LANES), F32),
            pltpu.VMEM((6, 8, LANES), F32), pltpu.VMEM((NY, 8, LANES), F32), pltpu.VMEM((NZ, 8, LANES), F32),
            pltpu.VMEM((NORM_ROWS, LANES), F32),
            dma((8,)), regular, regular((2,)), regular((3,)),
            dma((8,)), dma((PIECES,)), dma((PIECES,)), dma((2 + STRIPS,)), dma((5,)), dma((8,)), dma((4,)),
        ],
        compiler_params=pltpu.CompilerParams(
            collective_id=0, has_side_effects=True, vmem_limit_bytes=24 << 20),
    )(*(pltpu.with_memory_space_constraint(a, pltpu.HBM) for a in (tg.T, lg.T, hg, tu.T, lu.T, hu, nt, ns)))
    gate, up, col_g, col_u, norm = pl.pallas_call(
        write_kernel,
        name="write_results",
        out_shape=tuple(jax.ShapeDtypeStruct(*r) for r in results),
        in_specs=[vmem] * 5,
        out_specs=(hbm,) * 5,
        scratch_shapes=[dma((13,))],
        compiler_params=pltpu.CompilerParams(vmem_limit_bytes=4 << 20),
    )(*(pltpu.with_memory_space_constraint(a, pltpu.VMEM) for a in made))
    return gate.T, up.T, col_g.reshape(WIDE), col_u.reshape(WIDE), norm.reshape(D_MODEL)


def solution(mesh):
    return jax.shard_map(
        on_device,
        mesh=mesh,
        in_specs=(
            P("zero", "cols"), P("zero", None), P(None, "cols"),
            P("zero", "cols"), P("zero", None), P(None, "cols"),
            P(("zero", "cols")), P(("zero", "cols")),
        ),
        out_specs=(P(None, "cols"), P(None, "cols"), P("cols"), P("cols"), P()),
        check_vma=False,
    )
```

```python
import jax
import jax.numpy as jnp
from jax import lax
from jax.experimental import pallas as pl
from jax.experimental.pallas import tpu as pltpu
from jax.sharding import PartitionSpec as P

F32, BF16 = jnp.float32, jnp.bfloat16
MESH = pl.DeviceIdType.MESH

NX, NC, NY, NZ = 4, 2, 4, 16
GROUP = NX * NC
D_MODEL, WIDE, RANK = 5120, 400, 64
ROWS = D_MODEL // GROUP
LANES = 128
STRIPS = ROWS // LANES
MAIN, TAIL = 384, 16
STEP = 80
PER = 10
NORM_ROWS = D_MODEL // LANES

RAW = range(0, STRIPS)
UP = range(STRIPS, 2 * STRIPS)
PIECES = 2 * STRIPS
BY_PLUS = (0, 2, 4, 6, 8)
QUARTER = RANK // NY
OWN, LEFT, RIGHT, FAR = 0, 1, 2, 3


def gather_kernel(
    tg, lg, hg, tu, lu, hu, nt, ns,
    out_g, out_u, col_g, col_u, norm,
    raw, low, tuv, luv, hv, ht, ntv, nsv,
    lat, part, spread, sums, gbuf, ybuf, zbuf, nscr,
    load_sem, here, y_token, z_token,
    send, l_recv, r_recv, far_recv, d_recv, small_recv, n_send,
):
    me = lax.axis_index("zero")
    cols = lax.axis_index("cols")
    x, c = me // NC, me % NC
    z, y = cols // NY, cols % NY

    def chip(dx, core):
        return ((x + dx) % NX) * NC + core

    def at_x(dx, core):
        return (chip(dx, core), cols)

    def at_y(dy):
        return (me, z * NY + (y + dy) % NY)

    def at_z(dz):
        return (me, ((z + dz) % NZ) * NY + y)

    def signal(sem, dev):
        pl.semaphore_signal(sem, inc=1, device_id=dev, device_id_type=MESH)

    def copy_to(src, dst, send, recv, dev):
        return pltpu.make_async_remote_copy(
            src_ref=src, dst_ref=dst, send_sem=send, recv_sem=recv,
            device_id=dev, device_id_type=MESH)

    def remote(ref, send, recv, dev):
        return copy_to(ref, ref, send, recv, dev)

    partner = at_x(0, 1 - c)
    plus, minus, far = at_x(1, c), at_x(NX - 1, c), at_x(2, c)
    rail = [plus, minus, far]

    def lanes(shard, at=0, n=ROWS):
        return pl.ds(pl.multiple_of(shard * ROWS + at, LANES), n)

    mine = lanes(me)

    head = me == 0
    barrier = pltpu.get_barrier_semaphore()
    for peer in rail:
        signal(barrier, peer)

    @pl.when(c == 1)
    def _():
        signal(barrier, partner)

    loads = [
        pltpu.make_async_copy(a, b, load_sem.at[i])
        for i, (a, b) in enumerate(
            ((tg, raw.at[:, mine]), (nt, ntv), (ns, nsv), (hg, hv.at[0]), (lg, low.at[:, mine]),
             (hu, hv.at[1]), (lu, luv), (tu, tuv))
        )
    ]
    for load in loads:
        load.start()

    late = (z == 0) & (c == 0)
    for dy in (1, NY - 1):
        @pl.when((late & (y != 0)) | (jnp.logical_not(late) & ((y + dy) % NY != 0)))
        def _(dy=dy):
            signal(barrier, at_y(dy))

    for dz in (1, NZ - 1):
        @pl.when(head & ((z + dz) % NZ != 0))
        def _(dz=dz):
            signal(barrier, at_z(dz))

    source = [me, chip(NX - 1, c), chip(1, c), chip(2, c)]

    def piece(shard, n):
        if n in RAW:
            return raw.at[:, lanes(shard, n * LANES, LANES)]
        return out_u.at[:, lanes(shard, (n - STRIPS) * LANES, LANES)]

    def sent(n):
        return send.at[0 if n in RAW else 2]

    def by_plus(n, k=OWN):
        return remote(piece(source[k], n), sent(n), l_recv.at[n], plus)

    def by_minus(n, k=OWN):
        return remote(piece(source[k], n), sent(n), r_recv.at[n], minus)

    def onward(n, k=None):
        k, dev = (LEFT if k is None else k, plus) if n in BY_PLUS else (RIGHT if k is None else k, minus)
        return remote(piece(source[k], n), sent(n), far_recv.at[0 if n in RAW else n - STRIPS + 1], dev)

    def across(k, n):
        kind = 0 if n in RAW else 3
        return remote(piece(source[k], n), sent(n), d_recv.at[kind], partner)

    def crossed(ref, kind):
        return remote(ref, send.at[0], d_recv.at[kind], partner)

    def both_ways(n):
        by_plus(n).start()
        by_minus(n).start()

    def pass_on(n, now=True):
        def from_left():
            by_plus(n, LEFT).wait_recv()
            if n in BY_PLUS:
                onward(n).start()
            if now:
                across(LEFT, n).start()

        def from_right():
            by_minus(n, RIGHT).wait_recv()
            if n not in BY_PLUS:
                onward(n).start()
            if now:
                across(RIGHT, n).start()

        for step in (from_left, from_right) if n in BY_PLUS else (from_right, from_left):
            step()

    loads[0].wait()
    met = 4 - c + jnp.where(late, jnp.where(y % 2 == 0, 2, 1), jnp.where(y == 0, 0, 2))
    pl.semaphore_wait(barrier, met + jnp.where(head & (z != 0), 2, 0))
    both_ways(0)

    @pl.when(c == 0)
    def _():
        signal(here, partner)

    def y_tokens(i):
        for peer in (at_y(1), at_y(NY - 1)):
            signal(y_token.at[i], peer)

    @pl.when((late & (y == 0)) | (jnp.logical_not(late) & (y == 2)))
    def _():
        y_tokens(0)

    @pl.when(jnp.logical_not(late) & (y % 2 == 1))
    def _():
        y_tokens(1)

    @pl.when(head & (z != 0))
    def _():
        for peer in (at_z(1), at_z(NZ - 1)):
            signal(z_token.at[0], peer)

    loads[1].wait()
    loads[2].wait()
    row8 = lax.broadcasted_iota(jnp.int32, (8, LANES), 0)
    lane8 = lax.broadcasted_iota(jnp.int32, (8, LANES), 1)
    tile = jnp.zeros((8, LANES), F32)
    for k in range(PER):
        tile = jnp.where(lane8 == (cols * PER + k) % LANES, ntv[k] + nsv[k], tile)
    gbuf[x] = jnp.where(row8 == me, tile, 0.0)

    def gain_copy(i):
        return copy_to(gbuf.at[i], gbuf.at[i], send.at[3], small_recv.at[0], (c, cols))

    for i in range(1, NX):
        @pl.when(x == i)
        def _(i=i):
            gain_copy(i).start()

    def dot(a, b):
        return jnp.dot(a, b, preferred_element_type=F32)

    loads[3].wait()
    loads[5].wait()
    for k in range(2):
        ht[k] = (hv[k].astype(F32).T * 2.0).astype(BF16)
    part[WIDE + TAIL:512, :] = jnp.zeros((512 - WIDE - TAIL, LANES), F32)

    for k in range(2):
        loads[4 + 2 * k].wait()
        if k == 1:
            loads[7].wait()
        for q in range(WIDE // STEP):
            r = slice(STEP * q, STEP * q + STEP)
            if k == 0:
                w = raw[r, mine].astype(F32) + dot(ht[0, r, :], low[:, mine])
            else:
                w = tuv[r, :].astype(F32) + dot(ht[1, r, :], luv[...])
                lat[r, :] = w
            w = w * w
            s = w[:, 0:LANES]
            for t in range(1, STRIPS):
                s = s + w[:, LANES * t:LANES * t + LANES]
            if k == 0:
                part[r, :] = s
            elif r.stop <= MAIN:
                part[512 + r.start:512 + r.stop, :] = s
            else:
                part[512 + r.start:512 + MAIN, :] = s[:MAIN - r.start]
                part[WIDE:WIDE + TAIL, :] = s[MAIN - r.start:]

    sums[c * NX + x] = jnp.concatenate(
        [jnp.sum(part[LANES * t:LANES * t + LANES, :].T, axis=0, keepdims=True) for t in range(7)]
        + [jnp.zeros((1, LANES), F32)], axis=0)

    def sum_copy(peer, recv):
        return remote(sums.at[c * NX + x], send.at[4], small_recv.at[recv], peer)

    for peer in rail:
        sum_copy(peer, 1).start()
    quarter = pl.ds(pl.multiple_of(y * QUARTER, QUARTER), QUARTER)
    for peer in rail:
        remote(low.at[quarter, mine], send.at[1], small_recv.at[8], peer).start()
    for n in RAW[1:]:
        both_ways(n)

    def tokens(step):
        for peer in (at_z(1 << step), at_z(NZ - (1 << step))):
            signal(z_token.at[step], peer)

    @pl.when(head & (z != 0))
    def _():
        pl.semaphore_wait(z_token.at[0], 2)
        tokens(1)
        pl.semaphore_wait(z_token.at[1], 2)
        tokens(2)

    def first_tokens():
        pl.semaphore_wait(z_token.at[0], 2)
        tokens(0)
        tokens(1)

    @pl.when(head & (cols == 0))
    def _():
        first_tokens()

    eager = (cols == 0) & (c == 1)

    @pl.when(eager)
    def _():
        for n in RAW[:3]:
            pass_on(n, False)

    @pl.when(c == 1)
    def _():
        pl.semaphore_wait(here, 1)

    def gains_in():
        return remote(gbuf.at[pl.ds(0, 3)], send.at[3], small_recv.at[0], partner)

    def rail_gains():
        return (gbuf[0] + gbuf[1]) + (gbuf[2] + gbuf[3])

    def gains_over():
        return copy_to(gbuf.at[5], gbuf.at[4], send.at[3], small_recv.at[2], partner)

    @pl.when(me == 1)
    def _():
        gains_in().wait_recv()
        gbuf[5] = rail_gains()
        gains_over().start()

    remote(sums.at[pl.ds(0, 3)], send.at[4], small_recv.at[1], partner).wait_recv()
    rail_sums = remote(sums.at[pl.ds(c * NX, NX)], send.at[5], small_recv.at[3], partner)
    rail_sums.start()
    remote(raw.at[:, mine], send.at[0], d_recv.at[0], partner).start()
    remote(low.at[:, mine], send.at[1], d_recv.at[1], partner).start()
    remote(sums.at[pl.ds((1 - c) * NX, NX)], send.at[5], small_recv.at[3], partner).wait_recv()

    total = sums[0]
    for s in range(1, GROUP):
        total = total + sums[s % NC * NX + s // NC]
    column = jnp.sqrt(total)
    inverse = jnp.concatenate([1.0 / column, jnp.zeros((LANES - 8, LANES), F32)], axis=0).T

    def spread_out(k):
        for t in range(3):
            spread[k, LANES * t:LANES * t + LANES, :] = jnp.broadcast_to(
                inverse[:, 4 * k + t:4 * k + t + 1], (LANES, LANES))
        spread[k, MAIN:, :] = jnp.broadcast_to(
            inverse[TAIL * k:TAIL * k + TAIL, 3:4], (TAIL, LANES))

    spread_out(1)
    for n in UP:
        t = n - STRIPS
        out_u[:, lanes(me, t * LANES, LANES)] = (lat[:, t * LANES:t * LANES + LANES] * spread[1]).astype(BF16)
        both_ways(n)
        across(OWN, n).start()
    spread_out(0)

    col_g[...] = jnp.concatenate(
        [column[0:1], column[1:2], column[2:3], column[3:4]], axis=1)[:, :WIDE]
    col_u[...] = jnp.concatenate(
        [column[4:5], column[5:6], column[6:7], pltpu.roll(column, LANES - TAIL, axis=1)[3:4]], axis=1)[:, :WIDE]

    y_copies = [copy_to(ybuf.at[0], ybuf.at[i + 1], send.at[6], small_recv.at[4], at_y(dy))
                for i, dy in enumerate((1, NY - 1, 2))]

    def y_all():
        return remote(ybuf.at[pl.ds(0, 3)], send.at[6], small_recv.at[4], partner)

    def z_copy(d):
        return copy_to(zbuf.at[0], zbuf.at[d], send.at[7], small_recv.at[5], at_z(d))

    def z_all():
        return remote(zbuf.at[pl.ds(0, NZ - 1)], send.at[7], small_recv.at[5], partner)

    @pl.when(y % 2 == 1)
    def _():
        pl.semaphore_wait(y_token.at[0], 1)

    @pl.when(late & (y % 2 == 1))
    def _():
        y_tokens(1)

    @pl.when(y % 2 == 0)
    def _():
        pl.semaphore_wait(y_token.at[1], 2)

    def quarters(n, recv):
        return remote(low.at[pl.ds(0, n * QUARTER), pl.ds(0, 3 * ROWS)], send.at[1], small_recv.at[recv], partner)

    quarters(1, 8).wait_recv()
    for shard in source[1:]:
        for dy in (1, NY - 1, 2):
            remote(low.at[quarter, lanes(shard)], send.at[1], small_recv.at[9], at_y(dy)).start()

    @pl.when(head)
    def _():
        gains_in().wait_recv()
        gains_over().wait_recv()
        ybuf[0] = rail_gains() + gbuf[4]
        for copy in y_copies:
            copy.start()

    @pl.when(head & (z == 0) & (y != 0))
    def _():
        first_tokens()

    @pl.when(jnp.logical_not(eager))
    def _():
        for n in RAW[:3]:
            pass_on(n)

    @pl.when(head & (z == 0))
    def _():
        pl.semaphore_wait(z_token.at[1], 2)
        tokens(2)

    @pl.when(head)
    def _():
        y_all().wait_recv()
        zbuf[0] = (ybuf[0] + ybuf[1]) + (ybuf[2] + ybuf[3])

    def z_wave():
        pl.semaphore_wait(z_token.at[2], 2)
        for d in range(1, NZ):
            z_copy(d).start()

    @pl.when(head & (z != 0))
    def _():
        z_wave()

    @pl.when(eager)
    def _():
        for k in (LEFT, RIGHT):
            for n in RAW[:3]:
                across(k, n).start()

    for n in RAW[3:]:
        pass_on(n)

    quarters(NY - 1, 9).wait_recv()
    for shard in source[1:]:
        remote(low.at[:, lanes(shard)], send.at[1], d_recv.at[1], partner).start()
    crossed(raw.at[:, pl.ds(0, 3 * ROWS)], 0).wait_recv()
    crossed(low.at[:, pl.ds(0, 4 * ROWS)], 1).wait_recv()

    def finish(shard):
        w = lanes(shard)
        for q in range(WIDE // STEP):
            r = slice(STEP * q, STEP * q + STEP)
            s = spread[0, r, :]
            v = raw[r, w].astype(F32) + dot(ht[0, r, :], low[:, w])
            out_g[r, w] = (v * jnp.concatenate([s] * STRIPS, axis=1)).astype(BF16)

    def finish_near(i, _):
        d = i // NC
        finish(chip(d + d // 2, i % NC))
        return 0

    lax.fori_loop(0, 3 * NC, finish_near, 0)

    @pl.when(head & (z == 0))
    def _():
        z_wave()

    for n in UP[:2]:
        pass_on(n)

    def norm_copy(i, dev):
        return remote(norm, n_send.at[i], small_recv.at[7 if i == 3 else 6], dev)

    @pl.when(head)
    def _():
        z_all().wait_recv()
        tiles = [jnp.zeros((8, LANES), F32) for _ in range(5)]
        for d in range(NZ):
            start = ((z + NZ - d) % NZ) * NY * PER
            for t in range(5):
                place = lane8 + LANES * t
                tiles[t] = jnp.where((place >= start) & (place < start + NY * PER), zbuf[d], tiles[t])
        for t in range(5):
            nscr[pl.ds(t, 8, stride=5), :] = tiles[t]
        norm[...] = nscr[...].astype(BF16)

    for n in UP[2:3]:
        pass_on(n)

    @pl.when(head)
    def _():
        for i, dev in enumerate((*rail, partner)):
            norm_copy(i, dev).start()

    for n in UP[3:]:
        pass_on(n)

    far_lanes = lanes(source[FAR])
    remote(raw.at[:, far_lanes], send.at[0], far_recv.at[0], plus).wait_recv()
    remote(raw.at[:, far_lanes], send.at[0], d_recv.at[2], partner).start()
    crossed(raw.at[:, far_lanes], 2).wait_recv()

    def finish_far(i, _):
        finish(chip(2, i))
        return 0

    lax.fori_loop(0, NC, finish_far, 0)

    @pl.when((c == 0) & jnp.logical_not(head))
    def _():
        norm_copy(0, plus).wait_recv()
        norm_copy(3, partner).start()

    rail_sums.wait_send()
    remote(sums.at[pl.ds(0, 3)], send.at[4], small_recv.at[1], partner).wait_send()

    @pl.when((x > 0) | (me == 1))
    def _():
        gains_over().wait_send()

    @pl.when(head)
    def _():
        y_all().wait_send()
        z_all().wait_send()

    for n in UP[:-1]:
        onward(n, FAR).wait_recv()
        across(FAR, n).start()

    @pl.when(c == 1)
    def _():
        norm_copy(3, partner).wait_recv()

    @pl.when(c == 0)
    def _():
        norm_copy(3, partner).wait_send()

    @pl.when(head)
    def _():
        for i, dev in enumerate(rail):
            norm_copy(i, dev).wait_send()

    crossed(raw.at[:, pl.ds(0, 7 * ROWS)], 0).wait_send()
    remote(low.at[:, pl.ds(0, 7 * ROWS)], send.at[1], d_recv.at[1], partner).wait_send()

    for n in UP[-1:]:
        onward(n, FAR).wait_recv()
        across(FAR, n).start()
    remote(out_u.at[:, pl.ds(0, 7 * ROWS)], send.at[2], d_recv.at[3], partner).wait_send()
    crossed(out_u.at[:, pl.ds(0, 4 * ROWS)], 3).wait_recv()


def write_kernel(*refs):
    n = (len(refs) - 1) // 2
    sources, targets, sem = refs[:n], refs[n:2 * n], refs[2 * n]
    copies = []
    for src, dst in zip(sources, targets):
        tall = src.shape[0] == WIDE
        for q in range(WIDE // STEP if tall else 1):
            r = pl.ds(q * STEP, STEP) if tall else slice(None)
            copies.append(pltpu.make_async_copy(src.at[r, :], dst.at[r, :], sem.at[len(copies)]))
    for copy in copies:
        copy.start()
    for copy in copies:
        copy.wait()


def on_device(tg, lg, hg, tu, lu, hu, nt, ns):
    dma, regular = pltpu.SemaphoreType.DMA, pltpu.SemaphoreType.REGULAR
    hbm = pl.BlockSpec(memory_space=pltpu.HBM)
    vmem = pl.BlockSpec(memory_space=pltpu.VMEM)
    results = (
        ((WIDE, D_MODEL), BF16), ((WIDE, D_MODEL), BF16),
        ((1, WIDE), F32), ((1, WIDE), F32), ((NORM_ROWS, LANES), BF16),
    )
    made = pl.pallas_call(
        gather_kernel,
        name="gather_weights",
        out_shape=tuple(pltpu.VMEM(*r) for r in results),
        in_specs=[hbm] * 8,
        out_specs=(vmem,) * 5,
        scratch_shapes=[
            pltpu.VMEM((WIDE, D_MODEL), BF16), pltpu.VMEM((RANK, D_MODEL), BF16),
            pltpu.VMEM((WIDE, ROWS), BF16), pltpu.VMEM((RANK, ROWS), BF16),
            pltpu.VMEM((2, RANK, WIDE), BF16), pltpu.VMEM((2, WIDE, RANK), BF16),
            pltpu.SMEM((PER,), F32), pltpu.SMEM((PER,), F32),
            pltpu.VMEM((WIDE, ROWS), F32), pltpu.VMEM((7 * LANES, LANES), F32),
            pltpu.VMEM((2, WIDE, LANES), F32), pltpu.VMEM((GROUP, 8, LANES), F32),
            pltpu.VMEM((6, 8, LANES), F32), pltpu.VMEM((NY, 8, LANES), F32), pltpu.VMEM((NZ, 8, LANES), F32),
            pltpu.VMEM((NORM_ROWS, LANES), F32),
            dma((8,)), regular, regular((2,)), regular((3,)),
            dma((8,)), dma((PIECES,)), dma((PIECES,)), dma((1 + STRIPS,)), dma((4,)), dma((10,)), dma((4,)),
        ],
        compiler_params=pltpu.CompilerParams(
            collective_id=0, has_side_effects=True, vmem_limit_bytes=24 << 20),
    )(*(pltpu.with_memory_space_constraint(a, pltpu.HBM) for a in (tg.T, lg.T, hg, tu.T, lu.T, hu, nt, ns)))
    gate, up, col_g, col_u, norm = pl.pallas_call(
        write_kernel,
        name="write_results",
        out_shape=tuple(jax.ShapeDtypeStruct(*r) for r in results),
        in_specs=[vmem] * 5,
        out_specs=(hbm,) * 5,
        scratch_shapes=[dma((13,))],
        compiler_params=pltpu.CompilerParams(vmem_limit_bytes=4 << 20),
    )(*(pltpu.with_memory_space_constraint(a, pltpu.VMEM) for a in made))
    return gate.T, up.T, col_g.reshape(WIDE), col_u.reshape(WIDE), norm.reshape(D_MODEL)


def solution(mesh):
    return jax.shard_map(
        on_device,
        mesh=mesh,
        in_specs=(
            P("zero", "cols"), P("zero", None), P(None, "cols"),
            P("zero", "cols"), P("zero", None), P(None, "cols"),
            P(("zero", "cols")), P(("zero", "cols")),
        ),
        out_specs=(P(None, "cols"), P(None, "cols"), P("cols"), P("cols"), P()),
        check_vma=False,
    )
```

```python
import jax
import jax.numpy as jnp
from jax import lax
from jax.experimental import pallas as pl
from jax.experimental.pallas import tpu as pltpu
from jax.sharding import PartitionSpec as P

F32, BF16 = jnp.float32, jnp.bfloat16
MESH = pl.DeviceIdType.MESH

NX, NC, NY, NZ = 4, 2, 4, 16
GROUP = NX * NC
D_MODEL, WIDE, RANK = 5120, 400, 64
ROWS = D_MODEL // GROUP
LANES = 128
STRIPS = ROWS // LANES
MAIN, TAIL = 384, 16
STEP = 80
PER = 10
NORM_ROWS = D_MODEL // LANES

RAW = range(0, STRIPS)
UP = range(STRIPS, 2 * STRIPS)
PIECES = 2 * STRIPS
BY_PLUS = (0, 2, 4, 6, 8)
QUARTER = RANK // NY
OWN, LEFT, RIGHT, FAR = 0, 1, 2, 3


def gather_kernel(
    tg, lg, hg, tu, lu, hu, nt, ns,
    out_g, out_u, col_g, col_u, norm,
    raw, low, tuv, luv, hv, ht, ntv, nsv,
    lat, part, spread, sums, ybuf, zbuf, nscr,
    load_sem, here, y_token, z_token,
    send, l_recv, r_recv, far_recv, d_recv, small_recv, n_send,
):
    me = lax.axis_index("zero")
    cols = lax.axis_index("cols")
    x, c = me // NC, me % NC
    z, y = cols // NY, cols % NY

    def chip(dx, core):
        return ((x + dx) % NX) * NC + core

    def at_x(dx, core):
        return (chip(dx, core), cols)

    def at_y(dy):
        return (me, z * NY + (y + dy) % NY)

    def at_z(dz):
        return (me, ((z + dz) % NZ) * NY + y)

    def signal(sem, dev):
        pl.semaphore_signal(sem, inc=1, device_id=dev, device_id_type=MESH)

    def copy_to(src, dst, send, recv, dev):
        return pltpu.make_async_remote_copy(
            src_ref=src, dst_ref=dst, send_sem=send, recv_sem=recv,
            device_id=dev, device_id_type=MESH)

    def remote(ref, send, recv, dev):
        return copy_to(ref, ref, send, recv, dev)

    partner = at_x(0, 1 - c)
    plus, minus, far = at_x(1, c), at_x(NX - 1, c), at_x(2, c)
    rail = [plus, minus, far]

    def lanes(shard, at=0, n=ROWS):
        return pl.ds(pl.multiple_of(shard * ROWS + at, LANES), n)

    mine = lanes(me)

    head = c == 0
    first = pltpu.make_async_copy(
        tg.at[:, pl.ds(0, LANES)], raw.at[:, lanes(me, 0, LANES)], load_sem.at[8])
    first.start()
    barrier = pltpu.get_barrier_semaphore()
    for peer in rail:
        signal(barrier, peer)

    @pl.when(c == 1)
    def _():
        signal(barrier, partner)

    loads = [
        pltpu.make_async_copy(a, b, load_sem.at[i])
        for i, (a, b) in enumerate(
            ((tg.at[:, pl.ds(LANES, ROWS - LANES)], raw.at[:, lanes(me, LANES, ROWS - LANES)]), (nt, ntv), (ns, nsv), (hg, hv.at[0]), (lg, low.at[:, mine]),
             (hu, hv.at[1]), (lu, luv), (tu, tuv))
        )
    ]
    for load in loads:
        load.start()

    late = (z == 0) & head
    for dy in (1, NY - 1):
        @pl.when((late & (y != 0)) | (jnp.logical_not(late) & ((y + dy) % NY != 0)))
        def _(dy=dy):
            signal(barrier, at_y(dy))

    for dz in (1, NZ - 1):
        @pl.when(head & ((z + dz) % NZ != 0))
        def _(dz=dz):
            signal(barrier, at_z(dz))

    source = [me, chip(NX - 1, c), chip(1, c), chip(2, c)]

    def piece(shard, n):
        if n in RAW:
            return raw.at[:, lanes(shard, n * LANES, LANES)]
        return out_u.at[:, lanes(shard, (n - STRIPS) * LANES, LANES)]

    def sent(n):
        return send.at[0 if n in RAW else 2]

    def by_plus(n, k=OWN):
        return remote(piece(source[k], n), sent(n), l_recv.at[n], plus)

    def by_minus(n, k=OWN):
        return remote(piece(source[k], n), sent(n), r_recv.at[n], minus)

    def onward(n, k=None):
        k, dev = (LEFT if k is None else k, plus) if n in BY_PLUS else (RIGHT if k is None else k, minus)
        return remote(piece(source[k], n), sent(n), far_recv.at[0 if n in RAW else n - STRIPS + 1], dev)

    def across(k, n):
        kind = 0 if n in RAW else 3
        return remote(piece(source[k], n), sent(n), d_recv.at[kind], partner)

    def crossed(ref, kind):
        return remote(ref, send.at[0], d_recv.at[kind], partner)

    def both_ways(n):
        by_plus(n).start()
        by_minus(n).start()

    def pass_on(n, now=True):
        def from_left():
            by_plus(n, LEFT).wait_recv()
            if n in BY_PLUS:
                onward(n).start()
            if now:
                across(LEFT, n).start()

        def from_right():
            by_minus(n, RIGHT).wait_recv()
            if n not in BY_PLUS:
                onward(n).start()
            if now:
                across(RIGHT, n).start()

        for step in (from_left, from_right) if n in BY_PLUS else (from_right, from_left):
            step()

    first.wait()
    met = 4 - c + jnp.where(late, jnp.where(y % 2 == 0, 2, 1), jnp.where(y == 0, 0, 2))
    pl.semaphore_wait(barrier, met + jnp.where(head & (z != 0), 2, 0))
    both_ways(0)

    @pl.when(c == 0)
    def _():
        signal(here, partner)

    def y_tokens(i):
        for peer in (at_y(1), at_y(NY - 1)):
            signal(y_token.at[i], peer)

    @pl.when((late & (y == 0)) | (jnp.logical_not(late) & (y == 2)))
    def _():
        y_tokens(0)

    @pl.when(jnp.logical_not(late) & (y % 2 == 1))
    def _():
        y_tokens(1)

    @pl.when(head & (z != 0))
    def _():
        for peer in (at_z(1), at_z(NZ - 1)):
            signal(z_token.at[0], peer)

    def dot(a, b):
        return jnp.dot(a, b, preferred_element_type=F32)

    loads[0].wait()
    loads[3].wait()
    loads[5].wait()
    for k in range(2):
        ht[k] = (hv[k].astype(F32).T * 2.0).astype(BF16)
    part[WIDE + TAIL:512, :] = jnp.zeros((512 - WIDE - TAIL, LANES), F32)

    for k in range(2):
        loads[4 + 2 * k].wait()
        if k == 1:
            loads[7].wait()
        for q in range(WIDE // STEP):
            r = slice(STEP * q, STEP * q + STEP)
            if k == 0:
                w = raw[r, mine].astype(F32) + dot(ht[0, r, :], low[:, mine])
            else:
                w = tuv[r, :].astype(F32) + dot(ht[1, r, :], luv[...])
                lat[r, :] = w
            w = w * w
            s = w[:, 0:LANES]
            for t in range(1, STRIPS):
                s = s + w[:, LANES * t:LANES * t + LANES]
            if k == 0:
                part[r, :] = s
            elif r.stop <= MAIN:
                part[512 + r.start:512 + r.stop, :] = s
            else:
                part[512 + r.start:512 + MAIN, :] = s[:MAIN - r.start]
                part[WIDE:WIDE + TAIL, :] = s[MAIN - r.start:]

    loads[1].wait()
    loads[2].wait()
    lane = lax.broadcasted_iota(jnp.int32, (1, LANES), 1)
    own_gains = jnp.zeros((1, LANES), F32)
    for k in range(PER):
        own_gains = jnp.where(lane == (cols * PER + k) % LANES, ntv[k] + nsv[k], own_gains)

    sums[c * NX + x] = jnp.concatenate(
        [jnp.sum(part[LANES * t:LANES * t + LANES, :].T, axis=0, keepdims=True) for t in range(7)]
        + [own_gains], axis=0)

    def sum_copy(peer, recv):
        return remote(sums.at[c * NX + x], send.at[4], small_recv.at[recv], peer)

    for peer in rail:
        sum_copy(peer, 1).start()
    quarter = pl.ds(pl.multiple_of(y * QUARTER, QUARTER), QUARTER)
    for peer in (plus, minus):
        remote(low.at[quarter, mine], send.at[1], small_recv.at[8], peer).start()
    for n in RAW[1:]:
        both_ways(n)

    def tokens(step):
        for peer in (at_z(1 << step), at_z(NZ - (1 << step))):
            signal(z_token.at[step], peer)

    eager = (cols == 0) & (c == 1)

    @pl.when(eager)
    def _():
        for n in RAW[:4]:
            pass_on(n, False)

    @pl.when(c == 1)
    def _():
        pl.semaphore_wait(here, 1)

    remote(sums.at[pl.ds(0, 3)], send.at[4], small_recv.at[1], partner).wait_recv()
    rail_sums = remote(sums.at[pl.ds(c * NX, NX)], send.at[5], small_recv.at[3], partner)
    rail_sums.start()

    def low_block(rows, wide, recv):
        return remote(low.at[pl.ds(0, rows), pl.ds(0, wide * ROWS)], send.at[1], small_recv.at[recv], partner)

    low_block(QUARTER, 2, 8).wait_recv()
    for core, k, dev in ((0, LEFT, plus), (1, RIGHT, minus)):
        @pl.when(c == core)
        def _(k=k, dev=dev):
            remote(low.at[quarter, lanes(source[k])], send.at[1], small_recv.at[0], dev).start()

    remote(raw.at[:, mine], send.at[0], d_recv.at[0], partner).start()
    remote(low.at[:, mine], send.at[1], d_recv.at[1], partner).start()
    remote(sums.at[pl.ds((1 - c) * NX, NX)], send.at[5], small_recv.at[3], partner).wait_recv()

    total = sums[0]
    for s in range(1, GROUP):
        total = total + sums[s % NC * NX + s // NC]
    column = jnp.sqrt(total)
    inverse = jnp.concatenate([1.0 / column, jnp.zeros((LANES - 8, LANES), F32)], axis=0).T

    def spread_out(k):
        for t in range(3):
            spread[k, LANES * t:LANES * t + LANES, :] = jnp.broadcast_to(
                inverse[:, 4 * k + t:4 * k + t + 1], (LANES, LANES))
        spread[k, MAIN:, :] = jnp.broadcast_to(
            inverse[TAIL * k:TAIL * k + TAIL, 3:4], (TAIL, LANES))

    spread_out(1)
    for n in UP:
        t = n - STRIPS
        out_u[:, lanes(me, t * LANES, LANES)] = (lat[:, t * LANES:t * LANES + LANES] * spread[1]).astype(BF16)
        both_ways(n)
        across(OWN, n).start()
    spread_out(0)

    col_g[...] = jnp.concatenate(
        [column[0:1], column[1:2], column[2:3], column[3:4]], axis=1)[:, :WIDE]
    col_u[...] = jnp.concatenate(
        [column[4:5], column[5:6], column[6:7], pltpu.roll(column, LANES - TAIL, axis=1)[3:4]], axis=1)[:, :WIDE]

    y_copies = [copy_to(ybuf.at[0], ybuf.at[i + 1], send.at[6], small_recv.at[4], at_y(dy))
                for i, dy in enumerate((1, NY - 1, 2))]

    def y_all():
        return remote(ybuf.at[pl.ds(0, 3)], send.at[6], small_recv.at[4], partner)

    def z_copy(d):
        return copy_to(zbuf.at[0], zbuf.at[d], send.at[7], small_recv.at[5], at_z(d))

    def z_all():
        return remote(zbuf.at[pl.ds(0, NZ - 1)], send.at[7], small_recv.at[5], partner)

    @pl.when(y % 2 == 1)
    def _():
        pl.semaphore_wait(y_token.at[0], 1)

    @pl.when(late & (y % 2 == 1))
    def _():
        y_tokens(1)

    @pl.when(y % 2 == 0)
    def _():
        pl.semaphore_wait(y_token.at[1], 2)

    def share(k, recv):
        for dy in (1, NY - 1, 2):
            remote(low.at[quarter, lanes(source[k])], send.at[1], small_recv.at[recv], at_y(dy)).start()

    share(LEFT, 9)
    share(RIGHT, 9)

    @pl.when(head)
    def _():
        ybuf[0] = jnp.concatenate(
            [sums[s % NC * NX + s // NC][7:8, :] for s in range(GROUP)], axis=0)
        for copy in y_copies:
            copy.start()

    @pl.when(head & (z != 0))
    def _():
        pl.semaphore_wait(z_token.at[0], 2)
        tokens(1)
        pl.semaphore_wait(z_token.at[1], 2)
        tokens(2)

    @pl.when(late)
    def _():
        pl.semaphore_wait(z_token.at[0], 2)
        tokens(0)
        tokens(1)

    @pl.when(jnp.logical_not(eager))
    def _():
        for n in RAW[:3]:
            pass_on(n)

    @pl.when(late)
    def _():
        pl.semaphore_wait(z_token.at[1], 2)
        tokens(2)

    @pl.when(head)
    def _():
        y_all().wait_recv()
        zbuf[0] = (ybuf[0] + ybuf[1]) + (ybuf[2] + ybuf[3])

    def z_wave():
        pl.semaphore_wait(z_token.at[2], 2)
        for d in range(1, NZ):
            z_copy(d).start()

    @pl.when(head & (z != 0))
    def _():
        z_wave()

    @pl.when(eager)
    def _():
        for k in (LEFT, RIGHT):
            for n in RAW[:4]:
                across(k, n).start()

    @pl.when(jnp.logical_not(eager))
    def _():
        pass_on(RAW[3])

    pass_on(RAW[4])

    low_block(2 * QUARTER, 3, 9).wait_recv()
    for k in (LEFT, RIGHT):
        remote(low.at[:, lanes(source[k])], send.at[1], d_recv.at[1], partner).start()
    low_block(QUARTER, 1, 0).wait_recv()
    share(FAR, 2)
    crossed(raw.at[:, pl.ds(0, 3 * ROWS)], 0).wait_recv()
    crossed(low.at[:, pl.ds(0, 3 * ROWS)], 1).wait_recv()

    def finish(shard):
        w = lanes(shard)
        for q in range(WIDE // STEP):
            r = slice(STEP * q, STEP * q + STEP)
            s = spread[0, r, :]
            v = raw[r, w].astype(F32) + dot(ht[0, r, :], low[:, w])
            out_g[r, w] = (v * jnp.concatenate([s] * STRIPS, axis=1)).astype(BF16)

    def finish_near(i, _):
        d = i // NC
        finish(chip(d + d // 2, i % NC))
        return 0

    lax.fori_loop(0, 3 * NC, finish_near, 0)

    @pl.when(late)
    def _():
        z_wave()

    for n in UP[:2]:
        pass_on(n)

    def norm_copy():
        return remote(norm, n_send.at[0], small_recv.at[6], partner)

    def all_gains():
        z_all().wait_recv()
        lane8 = lax.broadcasted_iota(jnp.int32, (8, LANES), 1)
        tiles = [jnp.zeros((8, LANES), F32) for _ in range(5)]
        for d in range(NZ):
            start = ((z + NZ - d) % NZ) * NY * PER
            for t in range(5):
                place = lane8 + LANES * t
                tiles[t] = jnp.where((place >= start) & (place < start + NY * PER), zbuf[d], tiles[t])
        for t in range(5):
            nscr[pl.ds(t, 8, stride=5), :] = tiles[t]
        norm[...] = nscr[...].astype(BF16)

    @pl.when(head & (z != 0))
    def _():
        all_gains()

    for n in UP[2:]:
        pass_on(n)

    @pl.when(late)
    def _():
        all_gains()

    far_lanes = lanes(source[FAR])
    low_block(3 * QUARTER, 1, 2).wait_recv()
    remote(low.at[:, far_lanes], send.at[1], d_recv.at[4], partner).start()
    remote(raw.at[:, far_lanes], send.at[0], far_recv.at[0], plus).wait_recv()
    remote(raw.at[:, far_lanes], send.at[0], d_recv.at[2], partner).start()
    crossed(low.at[:, far_lanes], 4).wait_recv()
    crossed(raw.at[:, far_lanes], 2).wait_recv()

    def finish_far(i, _):
        finish(chip(2, i))
        return 0

    lax.fori_loop(0, NC, finish_far, 0)

    @pl.when(head)
    def _():
        norm_copy().start()

    rail_sums.wait_send()
    remote(sums.at[pl.ds(0, 3)], send.at[4], small_recv.at[1], partner).wait_send()

    @pl.when(head)
    def _():
        y_all().wait_send()
        z_all().wait_send()

    for n in UP[:-1]:
        onward(n, FAR).wait_recv()
        across(FAR, n).start()

    @pl.when(c == 1)
    def _():
        norm_copy().wait_recv()

    @pl.when(head)
    def _():
        norm_copy().wait_send()

    crossed(raw.at[:, pl.ds(0, 7 * ROWS)], 0).wait_send()
    remote(low.at[:, pl.ds(0, 7 * ROWS)], send.at[1], d_recv.at[1], partner).wait_send()

    for n in UP[-1:]:
        onward(n, FAR).wait_recv()
        across(FAR, n).start()
    remote(out_u.at[:, pl.ds(0, 7 * ROWS)], send.at[2], d_recv.at[3], partner).wait_send()
    crossed(out_u.at[:, pl.ds(0, 4 * ROWS)], 3).wait_recv()


def write_kernel(*refs):
    n = (len(refs) - 1) // 2
    sources, targets, sem = refs[:n], refs[n:2 * n], refs[2 * n]
    copies = []
    for src, dst in zip(sources, targets):
        tall = src.shape[0] == WIDE
        for q in range(WIDE // STEP if tall else 1):
            r = pl.ds(q * STEP, STEP) if tall else slice(None)
            copies.append(pltpu.make_async_copy(src.at[r, :], dst.at[r, :], sem.at[len(copies)]))
    for copy in copies:
        copy.start()
    for copy in copies:
        copy.wait()


def on_device(tg, lg, hg, tu, lu, hu, nt, ns):
    dma, regular = pltpu.SemaphoreType.DMA, pltpu.SemaphoreType.REGULAR
    hbm = pl.BlockSpec(memory_space=pltpu.HBM)
    vmem = pl.BlockSpec(memory_space=pltpu.VMEM)
    results = (
        ((WIDE, D_MODEL), BF16), ((WIDE, D_MODEL), BF16),
        ((1, WIDE), F32), ((1, WIDE), F32), ((NORM_ROWS, LANES), BF16),
    )
    made = pl.pallas_call(
        gather_kernel,
        name="gather_weights",
        out_shape=tuple(pltpu.VMEM(*r) for r in results),
        in_specs=[hbm] * 8,
        out_specs=(vmem,) * 5,
        scratch_shapes=[
            pltpu.VMEM((WIDE, D_MODEL), BF16), pltpu.VMEM((RANK, D_MODEL), BF16),
            pltpu.VMEM((WIDE, ROWS), BF16), pltpu.VMEM((RANK, ROWS), BF16),
            pltpu.VMEM((2, RANK, WIDE), BF16), pltpu.VMEM((2, WIDE, RANK), BF16),
            pltpu.SMEM((PER,), F32), pltpu.SMEM((PER,), F32),
            pltpu.VMEM((WIDE, ROWS), F32), pltpu.VMEM((7 * LANES, LANES), F32),
            pltpu.VMEM((2, WIDE, LANES), F32), pltpu.VMEM((GROUP, 8, LANES), F32),
            pltpu.VMEM((NY, 8, LANES), F32), pltpu.VMEM((NZ, 8, LANES), F32),
            pltpu.VMEM((NORM_ROWS, LANES), F32),
            dma((9,)), regular, regular((2,)), regular((3,)),
            dma((8,)), dma((PIECES,)), dma((PIECES,)), dma((1 + STRIPS,)), dma((5,)), dma((10,)), dma((1,)),
        ],
        compiler_params=pltpu.CompilerParams(
            collective_id=0, has_side_effects=True, vmem_limit_bytes=24 << 20),
    )(*(pltpu.with_memory_space_constraint(a, pltpu.HBM) for a in (tg.T, lg.T, hg, tu.T, lu.T, hu, nt, ns)))
    gate, up, col_g, col_u, norm = pl.pallas_call(
        write_kernel,
        name="write_results",
        out_shape=tuple(jax.ShapeDtypeStruct(*r) for r in results),
        in_specs=[vmem] * 5,
        out_specs=(hbm,) * 5,
        scratch_shapes=[dma((13,))],
        compiler_params=pltpu.CompilerParams(vmem_limit_bytes=4 << 20),
    )(*(pltpu.with_memory_space_constraint(a, pltpu.VMEM) for a in made))
    return gate.T, up.T, col_g.reshape(WIDE), col_u.reshape(WIDE), norm.reshape(D_MODEL)


def solution(mesh):
    return jax.shard_map(
        on_device,
        mesh=mesh,
        in_specs=(
            P("zero", "cols"), P("zero", None), P(None, "cols"),
            P("zero", "cols"), P("zero", None), P(None, "cols"),
            P(("zero", "cols")), P(("zero", "cols")),
        ),
        out_specs=(P(None, "cols"), P(None, "cols"), P("cols"), P("cols"), P()),
        check_vma=False,
    )
```

```python
import jax
import jax.numpy as jnp
from jax import lax
from jax.experimental import pallas as pl
from jax.experimental.pallas import tpu as pltpu
from jax.sharding import PartitionSpec as P

F32, BF16 = jnp.float32, jnp.bfloat16
MESH = pl.DeviceIdType.MESH

NX, NC, NY, NZ = 4, 2, 4, 16
GROUP = NX * NC
D_MODEL, WIDE, RANK = 5120, 400, 64
ROWS = D_MODEL // GROUP
LANES = 128
STRIPS = ROWS // LANES
MAIN, TAIL = 384, 16
STEP = 80
PER = 10
NORM_ROWS = D_MODEL // LANES

RAW = range(0, 3)
UP = range(3, 3 + STRIPS)
PIECES = 3 + STRIPS
BY_PLUS = (0, 1, 4, 6)
QUARTER = RANK // NY
OWN, LEFT, RIGHT, FAR = 0, 1, 2, 3


def gather_kernel(
    tg, lg, hg, tu, lu, hu, nt, ns,
    out_g, out_u, col_g, col_u, norm,
    raw, low, tuv, luv, hv, ht, ntv, nsv,
    lat, part, spread, sums, ybuf, zbuf, nscr,
    load_sem, here, y_token, z_token,
    send, l_recv, r_recv, far_recv, d_recv, small_recv, n_send,
):
    me = lax.axis_index("zero")
    cols = lax.axis_index("cols")
    x, c = me // NC, me % NC
    z, y = cols // NY, cols % NY

    def chip(dx, core):
        return ((x + dx) % NX) * NC + core

    def at_x(dx, core):
        return (chip(dx, core), cols)

    def at_y(dy):
        return (me, z * NY + (y + dy) % NY)

    def at_z(dz):
        return (me, ((z + dz) % NZ) * NY + y)

    def signal(sem, dev):
        pl.semaphore_signal(sem, inc=1, device_id=dev, device_id_type=MESH)

    def copy_to(src, dst, send, recv, dev):
        return pltpu.make_async_remote_copy(
            src_ref=src, dst_ref=dst, send_sem=send, recv_sem=recv,
            device_id=dev, device_id_type=MESH)

    def remote(ref, send, recv, dev):
        return copy_to(ref, ref, send, recv, dev)

    partner = at_x(0, 1 - c)
    plus, minus, far = at_x(1, c), at_x(NX - 1, c), at_x(2, c)
    rail = [plus, minus, far]

    def lanes(shard, at=0, n=ROWS):
        return pl.ds(pl.multiple_of(shard * ROWS + at, LANES), n)

    mine = lanes(me)

    head = c == 0
    first = pltpu.make_async_copy(
        tg.at[:, pl.ds(0, LANES)], raw.at[:, lanes(me, 0, LANES)], load_sem.at[8])
    first.start()
    barrier = pltpu.get_barrier_semaphore()
    for peer in rail:
        signal(barrier, peer)

    @pl.when(c == 1)
    def _():
        signal(barrier, partner)

    loads = [
        pltpu.make_async_copy(a, b, load_sem.at[i])
        for i, (a, b) in enumerate(
            ((tg.at[:, pl.ds(LANES, ROWS - LANES)], raw.at[:, lanes(me, LANES, ROWS - LANES)]), (nt, ntv), (ns, nsv), (hg, hv.at[0]), (lg, low.at[:, mine]),
             (hu, hv.at[1]), (lu, luv), (tu, tuv))
        )
    ]
    for load in loads:
        load.start()

    late = (z == 0) & head
    for dy in (1, NY - 1):
        @pl.when((late & (y != 0)) | (jnp.logical_not(late) & ((y + dy) % NY != 0)))
        def _(dy=dy):
            signal(barrier, at_y(dy))

    for dz in (1, NZ - 1):
        @pl.when(head & ((z + dz) % NZ != 0))
        def _(dz=dz):
            signal(barrier, at_z(dz))

    source = [me, chip(NX - 1, c), chip(1, c), chip(2, c)]

    def piece(shard, n):
        if n in RAW:
            return raw.at[:, lanes(shard, max(2 * n - 1, 0) * LANES, (2 if n else 1) * LANES)]
        return out_u.at[:, lanes(shard, (n - UP[0]) * LANES, LANES)]

    def sent(n):
        return send.at[0 if n in RAW else 2]

    def by_plus(n, k=OWN):
        return remote(piece(source[k], n), sent(n), l_recv.at[n], plus)

    def by_minus(n, k=OWN):
        return remote(piece(source[k], n), sent(n), r_recv.at[n], minus)

    def onward(n, k=None):
        k, dev = (LEFT if k is None else k, plus) if n in BY_PLUS else (RIGHT if k is None else k, minus)
        return remote(piece(source[k], n), sent(n), far_recv.at[0 if n in RAW else n - UP[0] + 1], dev)

    def across(k, n):
        kind = 0 if n in RAW else 3
        return remote(piece(source[k], n), sent(n), d_recv.at[kind], partner)

    def crossed(ref, kind):
        return remote(ref, send.at[0], d_recv.at[kind], partner)

    def both_ways(n):
        by_plus(n).start()
        by_minus(n).start()

    def pass_on(n, now=True):
        def from_left():
            by_plus(n, LEFT).wait_recv()
            if n in BY_PLUS:
                onward(n).start()
            if now:
                across(LEFT, n).start()

        def from_right():
            by_minus(n, RIGHT).wait_recv()
            if n not in BY_PLUS:
                onward(n).start()
            if now:
                across(RIGHT, n).start()

        for step in (from_left, from_right) if n in BY_PLUS else (from_right, from_left):
            step()

    first.wait()
    met = 4 - c + jnp.where(late, jnp.where(y % 2 == 0, 2, 1), jnp.where(y == 0, 0, 2))
    pl.semaphore_wait(barrier, met + jnp.where(head & (z != 0), 2, 0))
    both_ways(0)

    @pl.when(c == 0)
    def _():
        signal(here, partner)

    def y_tokens(i):
        for peer in (at_y(1), at_y(NY - 1)):
            signal(y_token.at[i], peer)

    @pl.when((late & (y == 0)) | (jnp.logical_not(late) & (y == 2)))
    def _():
        y_tokens(0)

    @pl.when(jnp.logical_not(late) & (y % 2 == 1))
    def _():
        y_tokens(1)

    @pl.when(head & (z != 0))
    def _():
        for peer in (at_z(1), at_z(NZ - 1)):
            signal(z_token.at[0], peer)

    def dot(a, b):
        return jnp.dot(a, b, preferred_element_type=F32)

    loads[0].wait()
    loads[3].wait()
    loads[5].wait()
    for k in range(2):
        ht[k] = (hv[k].astype(F32).T * 2.0).astype(BF16)
    part[WIDE + TAIL:512, :] = jnp.zeros((512 - WIDE - TAIL, LANES), F32)

    for k in range(2):
        loads[4 + 2 * k].wait()
        if k == 1:
            loads[7].wait()
        for q in range(WIDE // STEP):
            r = slice(STEP * q, STEP * q + STEP)
            if k == 0:
                w = raw[r, mine].astype(F32) + dot(ht[0, r, :], low[:, mine])
            else:
                w = tuv[r, :].astype(F32) + dot(ht[1, r, :], luv[...])
                lat[r, :] = w
            w = w * w
            s = w[:, 0:LANES]
            for t in range(1, STRIPS):
                s = s + w[:, LANES * t:LANES * t + LANES]
            if k == 0:
                part[r, :] = s
            elif r.stop <= MAIN:
                part[512 + r.start:512 + r.stop, :] = s
            else:
                part[512 + r.start:512 + MAIN, :] = s[:MAIN - r.start]
                part[WIDE:WIDE + TAIL, :] = s[MAIN - r.start:]

    loads[1].wait()
    loads[2].wait()
    lane = lax.broadcasted_iota(jnp.int32, (1, LANES), 1)
    own_gains = jnp.zeros((1, LANES), F32)
    for k in range(PER):
        own_gains = jnp.where(lane == (cols * PER + k) % LANES, ntv[k] + nsv[k], own_gains)

    sums[c * NX + x] = jnp.concatenate(
        [jnp.sum(part[LANES * t:LANES * t + LANES, :].T, axis=0, keepdims=True) for t in range(7)]
        + [own_gains], axis=0)

    def sum_copy(peer, recv):
        return remote(sums.at[c * NX + x], send.at[4], small_recv.at[recv], peer)

    for peer in rail:
        sum_copy(peer, 1).start()
    quarter = pl.ds(pl.multiple_of(y * QUARTER, QUARTER), QUARTER)
    for peer in (plus, minus):
        remote(low.at[quarter, mine], send.at[1], small_recv.at[8], peer).start()
    for n in RAW[1:]:
        both_ways(n)

    def tokens(step):
        for peer in (at_z(1 << step), at_z(NZ - (1 << step))):
            signal(z_token.at[step], peer)

    eager = (cols == 0) & (c == 1)

    @pl.when(eager)
    def _():
        for n in RAW[:2]:
            pass_on(n, False)

    @pl.when(c == 1)
    def _():
        pl.semaphore_wait(here, 1)

    remote(sums.at[pl.ds(0, 3)], send.at[4], small_recv.at[1], partner).wait_recv()
    rail_sums = remote(sums.at[pl.ds(c * NX, NX)], send.at[5], small_recv.at[3], partner)
    rail_sums.start()

    def low_block(rows, wide, recv):
        return remote(low.at[pl.ds(0, rows), pl.ds(0, wide * ROWS)], send.at[1], small_recv.at[recv], partner)

    low_block(QUARTER, 2, 8).wait_recv()
    for core, k, dev in ((0, LEFT, plus), (1, RIGHT, minus)):
        @pl.when(c == core)
        def _(k=k, dev=dev):
            remote(low.at[quarter, lanes(source[k])], send.at[1], small_recv.at[0], dev).start()

    remote(raw.at[:, mine], send.at[0], d_recv.at[0], partner).start()
    remote(low.at[:, mine], send.at[1], d_recv.at[1], partner).start()
    remote(sums.at[pl.ds((1 - c) * NX, NX)], send.at[5], small_recv.at[3], partner).wait_recv()

    total = sums[0]
    for s in range(1, GROUP):
        total = total + sums[s % NC * NX + s // NC]
    column = jnp.sqrt(total)
    inverse = jnp.concatenate([1.0 / column, jnp.zeros((LANES - 8, LANES), F32)], axis=0).T

    def spread_out(k):
        for t in range(3):
            spread[k, LANES * t:LANES * t + LANES, :] = jnp.broadcast_to(
                inverse[:, 4 * k + t:4 * k + t + 1], (LANES, LANES))
        spread[k, MAIN:, :] = jnp.broadcast_to(
            inverse[TAIL * k:TAIL * k + TAIL, 3:4], (TAIL, LANES))

    spread_out(1)
    for n in UP:
        t = n - UP[0]
        out_u[:, lanes(me, t * LANES, LANES)] = (lat[:, t * LANES:t * LANES + LANES] * spread[1]).astype(BF16)
        both_ways(n)
        across(OWN, n).start()
    spread_out(0)

    col_g[...] = jnp.concatenate(
        [column[0:1], column[1:2], column[2:3], column[3:4]], axis=1)[:, :WIDE]
    col_u[...] = jnp.concatenate(
        [column[4:5], column[5:6], column[6:7], pltpu.roll(column, LANES - TAIL, axis=1)[3:4]], axis=1)[:, :WIDE]

    y_copies = [copy_to(ybuf.at[0], ybuf.at[i + 1], send.at[6], small_recv.at[4], at_y(dy))
                for i, dy in enumerate((1, NY - 1, 2))]

    def y_all():
        return remote(ybuf.at[pl.ds(0, 3)], send.at[6], small_recv.at[4], partner)

    def z_copy(d):
        return copy_to(zbuf.at[0], zbuf.at[d], send.at[7], small_recv.at[5], at_z(d))

    def z_all():
        return remote(zbuf.at[pl.ds(0, NZ - 1)], send.at[7], small_recv.at[5], partner)

    @pl.when(y % 2 == 1)
    def _():
        pl.semaphore_wait(y_token.at[0], 1)

    @pl.when(late & (y % 2 == 1))
    def _():
        y_tokens(1)

    @pl.when(y % 2 == 0)
    def _():
        pl.semaphore_wait(y_token.at[1], 2)

    def share(k, recv):
        for dy in (1, NY - 1, 2):
            remote(low.at[quarter, lanes(source[k])], send.at[1], small_recv.at[recv], at_y(dy)).start()

    share(LEFT, 9)
    share(RIGHT, 9)

    @pl.when(head)
    def _():
        ybuf[0] = jnp.concatenate(
            [sums[s % NC * NX + s // NC][7:8, :] for s in range(GROUP)], axis=0)
        for copy in y_copies:
            copy.start()

    @pl.when(head & (z != 0))
    def _():
        pl.semaphore_wait(z_token.at[0], 2)
        tokens(1)
        pl.semaphore_wait(z_token.at[1], 2)
        tokens(2)

    @pl.when(late)
    def _():
        pl.semaphore_wait(z_token.at[0], 2)
        tokens(0)
        tokens(1)

    @pl.when(jnp.logical_not(eager))
    def _():
        for n in RAW[:2]:
            pass_on(n)

    @pl.when(late)
    def _():
        pl.semaphore_wait(z_token.at[1], 2)
        tokens(2)

    @pl.when(head)
    def _():
        y_all().wait_recv()
        zbuf[0] = (ybuf[0] + ybuf[1]) + (ybuf[2] + ybuf[3])

    def z_wave():
        pl.semaphore_wait(z_token.at[2], 2)
        for d in range(1, NZ):
            z_copy(d).start()

    @pl.when(head & (z != 0))
    def _():
        z_wave()

    @pl.when(eager)
    def _():
        for k in (LEFT, RIGHT):
            for n in RAW[:2]:
                across(k, n).start()

    pass_on(RAW[2])

    low_block(2 * QUARTER, 3, 9).wait_recv()
    for k in (LEFT, RIGHT):
        remote(low.at[:, lanes(source[k])], send.at[1], d_recv.at[1], partner).start()
    low_block(QUARTER, 1, 0).wait_recv()
    share(FAR, 2)
    crossed(raw.at[:, pl.ds(0, 3 * ROWS)], 0).wait_recv()
    crossed(low.at[:, pl.ds(0, 3 * ROWS)], 1).wait_recv()

    def finish(shard):
        w = lanes(shard)
        for q in range(WIDE // STEP):
            r = slice(STEP * q, STEP * q + STEP)
            s = spread[0, r, :]
            v = raw[r, w].astype(F32) + dot(ht[0, r, :], low[:, w])
            out_g[r, w] = (v * jnp.concatenate([s] * STRIPS, axis=1)).astype(BF16)

    def finish_near(i, _):
        d = i // NC
        finish(chip(d + d // 2, i % NC))
        return 0

    lax.fori_loop(0, 3 * NC, finish_near, 0)

    @pl.when(late)
    def _():
        z_wave()

    for n in UP[:2]:
        pass_on(n)

    def norm_copy():
        return remote(norm, n_send.at[0], small_recv.at[6], partner)

    def all_gains():
        z_all().wait_recv()
        lane8 = lax.broadcasted_iota(jnp.int32, (8, LANES), 1)
        tiles = [jnp.zeros((8, LANES), F32) for _ in range(5)]
        for d in range(NZ):
            start = ((z + NZ - d) % NZ) * NY * PER
            for t in range(5):
                place = lane8 + LANES * t
                tiles[t] = jnp.where((place >= start) & (place < start + NY * PER), zbuf[d], tiles[t])
        for t in range(5):
            nscr[pl.ds(t, 8, stride=5), :] = tiles[t]
        norm[...] = nscr[...].astype(BF16)

    @pl.when(head & (z != 0))
    def _():
        all_gains()

    for n in UP[2:]:
        pass_on(n)

    @pl.when(late)
    def _():
        all_gains()

    far_lanes = lanes(source[FAR])
    low_block(3 * QUARTER, 1, 2).wait_recv()
    remote(low.at[:, far_lanes], send.at[1], d_recv.at[4], partner).start()
    remote(raw.at[:, far_lanes], send.at[0], far_recv.at[0], plus).wait_recv()
    remote(raw.at[:, far_lanes], send.at[0], d_recv.at[2], partner).start()
    crossed(low.at[:, far_lanes], 4).wait_recv()
    crossed(raw.at[:, far_lanes], 2).wait_recv()

    def finish_far(i, _):
        finish(chip(2, i))
        return 0

    lax.fori_loop(0, NC, finish_far, 0)

    @pl.when(head)
    def _():
        norm_copy().start()

    rail_sums.wait_send()
    remote(sums.at[pl.ds(0, 3)], send.at[4], small_recv.at[1], partner).wait_send()

    @pl.when(head)
    def _():
        y_all().wait_send()
        z_all().wait_send()

    for n in UP[:-1]:
        onward(n, FAR).wait_recv()
        across(FAR, n).start()

    @pl.when(c == 1)
    def _():
        norm_copy().wait_recv()

    @pl.when(head)
    def _():
        norm_copy().wait_send()

    crossed(raw.at[:, pl.ds(0, 7 * ROWS)], 0).wait_send()
    remote(low.at[:, pl.ds(0, 7 * ROWS)], send.at[1], d_recv.at[1], partner).wait_send()

    for n in UP[-1:]:
        onward(n, FAR).wait_recv()
        across(FAR, n).start()
    remote(out_u.at[:, pl.ds(0, 7 * ROWS)], send.at[2], d_recv.at[3], partner).wait_send()
    crossed(out_u.at[:, pl.ds(0, 4 * ROWS)], 3).wait_recv()


def write_kernel(*refs):
    n = (len(refs) - 1) // 2
    sources, targets, sem = refs[:n], refs[n:2 * n], refs[2 * n]
    copies = []
    for src, dst in zip(sources, targets):
        tall = src.shape[0] == WIDE
        for q in range(WIDE // STEP if tall else 1):
            r = pl.ds(q * STEP, STEP) if tall else slice(None)
            copies.append(pltpu.make_async_copy(src.at[r, :], dst.at[r, :], sem.at[len(copies)]))
    for copy in copies:
        copy.start()
    for copy in copies:
        copy.wait()


def on_device(tg, lg, hg, tu, lu, hu, nt, ns):
    dma, regular = pltpu.SemaphoreType.DMA, pltpu.SemaphoreType.REGULAR
    hbm = pl.BlockSpec(memory_space=pltpu.HBM)
    vmem = pl.BlockSpec(memory_space=pltpu.VMEM)
    results = (
        ((WIDE, D_MODEL), BF16), ((WIDE, D_MODEL), BF16),
        ((1, WIDE), F32), ((1, WIDE), F32), ((NORM_ROWS, LANES), BF16),
    )
    made = pl.pallas_call(
        gather_kernel,
        name="gather_weights",
        out_shape=tuple(pltpu.VMEM(*r) for r in results),
        in_specs=[hbm] * 8,
        out_specs=(vmem,) * 5,
        scratch_shapes=[
            pltpu.VMEM((WIDE, D_MODEL), BF16), pltpu.VMEM((RANK, D_MODEL), BF16),
            pltpu.VMEM((WIDE, ROWS), BF16), pltpu.VMEM((RANK, ROWS), BF16),
            pltpu.VMEM((2, RANK, WIDE), BF16), pltpu.VMEM((2, WIDE, RANK), BF16),
            pltpu.SMEM((PER,), F32), pltpu.SMEM((PER,), F32),
            pltpu.VMEM((WIDE, ROWS), F32), pltpu.VMEM((7 * LANES, LANES), F32),
            pltpu.VMEM((2, WIDE, LANES), F32), pltpu.VMEM((GROUP, 8, LANES), F32),
            pltpu.VMEM((NY, 8, LANES), F32), pltpu.VMEM((NZ, 8, LANES), F32),
            pltpu.VMEM((NORM_ROWS, LANES), F32),
            dma((9,)), regular, regular((2,)), regular((3,)),
            dma((8,)), dma((PIECES,)), dma((PIECES,)), dma((1 + STRIPS,)), dma((5,)), dma((10,)), dma((1,)),
        ],
        compiler_params=pltpu.CompilerParams(
            collective_id=0, has_side_effects=True, vmem_limit_bytes=24 << 20),
    )(*(pltpu.with_memory_space_constraint(a, pltpu.HBM) for a in (tg.T, lg.T, hg, tu.T, lu.T, hu, nt, ns)))
    gate, up, col_g, col_u, norm = pl.pallas_call(
        write_kernel,
        name="write_results",
        out_shape=tuple(jax.ShapeDtypeStruct(*r) for r in results),
        in_specs=[vmem] * 5,
        out_specs=(hbm,) * 5,
        scratch_shapes=[dma((13,))],
        compiler_params=pltpu.CompilerParams(vmem_limit_bytes=4 << 20),
    )(*(pltpu.with_memory_space_constraint(a, pltpu.VMEM) for a in made))
    return gate.T, up.T, col_g.reshape(WIDE), col_u.reshape(WIDE), norm.reshape(D_MODEL)


def solution(mesh):
    return jax.shard_map(
        on_device,
        mesh=mesh,
        in_specs=(
            P("zero", "cols"), P("zero", None), P(None, "cols"),
            P("zero", "cols"), P("zero", None), P(None, "cols"),
            P(("zero", "cols")), P(("zero", "cols")),
        ),
        out_specs=(P(None, "cols"), P(None, "cols"), P("cols"), P("cols"), P()),
        check_vma=False,
    )
```
